256 devices in a mesh: gx: 4 (over z_lo), gy: 8 (over y, z_hi), gz: 8 (over x, core).
Axes of the slice: x: 4, y: 4, z: 8 (z_hi: 2, z_lo: 4; z = z_hi * 4 + z_lo), core: 2. Of those that a mesh axis runs over, the one named last changes fastest.
Arguments:
- displ: float32 [3, 4, 8, 8, 9945], P(None, 'gx', 'gy', 'gz'), may hold values from -6 to 6
- veloc: float32 [3, 4, 8, 8, 9945], P(None, 'gx', 'gy', 'gz'), may hold values from -6 to 6
- accel: float32 [3, 4, 8, 8, 9945], P(None, 'gx', 'gy', 'gz'), may hold values from -12 to 12
- node_index: int32 [4, 8, 8, 125, 128], P('gx', 'gy', 'gz'), may hold values from 0 to 9944, as said below
- inv_map: float32 [4, 8, 8, 9, 125, 128], P('gx', 'gy', 'gz'), may hold values from -1 to 2, as said below
- jac_weight: float32 [4, 8, 8, 125, 128], P('gx', 'gy', 'gz'), may hold values from 0.05 to 0.5
- lame_first: float32 [4, 8, 8, 125, 128], P('gx', 'gy', 'gz'), may hold values from 0.02 to 0.1
- shear_mod: float32 [4, 8, 8, 125, 128], P('gx', 'gy', 'gz'), may hold values from 0.02 to 0.1
- density: float32 [4, 8, 8, 125, 128], P('gx', 'gy', 'gz'), may hold values from 1 to 3
Outputs:
- displ_out: float32 [3, 4, 8, 8, 9945], P(None, 'gx', 'gy', 'gz')
- veloc_out: float32 [3, 4, 8, 8, 9945], P(None, 'gx', 'gy', 'gz')
- accel_out: float32 [3, 4, 8, 8, 9945], P(None, 'gx', 'gy', 'gz')
The draws below stay inside these ranges and needn't reach their ends.
Inputs may be any that keep to these rules, and one draw needn't show every extreme that they name: `node_index`: on each device the element slots hold the elements of a brick of 4 x 16 x 2 elements in a drawn order, each once; element (ex, ey, ez) has its point (a, b, c) at node ((4 ex + a) * 65 + 4 ey + b) * 9 + 4 ez + c. `inv_map`: the entries with l equal to j are positive.
All inputs are finite; a program needn't handle non-finite values.
Results may differ from the reference program's by a relative error of at most 0.00024.
Values sent between devices are 32-bit elements; how exact they have to be, the bound alone decides.
No kernel may reach another device: no remote copies, remote signals or barrier semaphores. Data moves between devices by JAX's collectives and lax.ppermute only.
A program may use at most 64 MiB of HBM per device.

```python
import math
import jax
import jax.numpy as jnp
import numpy as np
from jax import lax

NGLL = 5
EX = 4
EY = 16
EZ = 2
STEPS = 1
E_DEV = 128
NODES_DEV = 9945
N_GX = 4
N_GY = 8
N_GZ = 8


def draw_node_index(key, part):
    devices = N_GX * N_GY * N_GZ
    elements = EX * EY * EZ
    keys = jax.random.split(key, devices)
    orders = jax.vmap(lambda subkey: jax.random.permutation(subkey, elements))(keys).astype(jnp.int32)
    elem_x = orders // (EY * EZ)
    elem_y = orders // EZ % EY
    elem_z = orders % EZ
    points = jnp.arange(125, dtype=jnp.int32)
    offset_a = points // 25
    offset_b = points // 5 % 5
    offset_c = points % 5
    node_y = 4 * EY + 1
    node_z = 4 * EZ + 1
    along_x = 4 * elem_x[:, None, :] + offset_a[None, :, None]
    along_y = 4 * elem_y[:, None, :] + offset_b[None, :, None]
    along_z = 4 * elem_z[:, None, :] + offset_c[None, :, None]
    flat = (along_x * node_y + along_y) * node_z + along_z
    return flat.reshape(N_GX, N_GY, N_GZ, 125, elements).astype(jnp.int32)


def draw_inv_map(key, part):
    elements = EX * EY * EZ
    shape = (N_GX, N_GY, N_GZ, 3, 3, 125, elements)
    diag_key, other_key = jax.random.split(key)
    diagonal = jax.random.uniform(diag_key, shape, jnp.float32, 0.7, 1.4)
    offdiag = jnp.clip(0.25 * jax.random.normal(other_key, shape, jnp.float32), -1.0, 1.0)
    identity = jnp.eye(3, dtype=jnp.float32)[:, :, None, None]
    full = identity * diagonal + (1.0 - identity) * offdiag
    return full.reshape(N_GX, N_GY, N_GZ, 9, 125, elements).astype(jnp.float32)


def block_levels(stream_key, dims, pieces, low, largest):
    loudness, own = 1.0, jax.random.fold_in(stream_key, 6)
    for axis_at, blocks in pieces:
        draws = jnp.exp(jax.random.uniform(jax.random.fold_in(own, axis_at), (blocks,), jnp.float32, low / len(pieces), largest / len(pieces)))
        loudness = loudness * jnp.repeat(draws, dims[axis_at] // blocks).reshape([-1 if axis == axis_at else 1 for axis in range(len(dims))])
    return loudness


def normal_values(key, extent, width, limit, shards=(), kind=jnp.bfloat16):
    values = width * jax.random.normal(key, extent, jnp.float32)
    if shards:
        values = values * block_levels(key, extent, shards, -0.22, 0.18)
    return jnp.clip(values, -limit, limit).astype(kind)


def setup_inputs(seed: int = 0) -> dict:
    seeds = jax.random.split(jax.random.key(seed), 10)
    return {
        "displ": normal_values(seeds[0], (3, N_GX, N_GY, N_GZ, NODES_DEV), 1.0, 6.0, ((1, 4), (2, 8), (3, 8)), jnp.float32),
        "veloc": normal_values(seeds[1], (3, N_GX, N_GY, N_GZ, NODES_DEV), 1.0, 6.0, ((1, 4), (2, 8), (3, 8)), jnp.float32),
        "accel": normal_values(seeds[2], (3, N_GX, N_GY, N_GZ, NODES_DEV), 2.0, 12.0, ((1, 4), (2, 8), (3, 8)), jnp.float32),
        "node_index": draw_node_index(jax.random.fold_in(seeds[9], 71), 0),
        "inv_map": draw_inv_map(jax.random.fold_in(seeds[9], 71), 0),
        "jac_weight": jnp.clip(jnp.exp(math.log(0.5) - 2.3025851 * jax.random.uniform(seeds[5], (N_GX, N_GY, N_GZ, NGLL * NGLL * NGLL, E_DEV), jnp.float32) ** block_levels(seeds[5], (N_GX, N_GY, N_GZ, NGLL * NGLL * NGLL, E_DEV), ((0, 4), (1, 8), (2, 8)), -0.2, 0.2)), 0.05, 0.5),
        "lame_first": jnp.clip(jnp.exp(math.log(0.1) - 1.609438 * jax.random.uniform(seeds[6], (N_GX, N_GY, N_GZ, NGLL * NGLL * NGLL, E_DEV), jnp.float32) ** block_levels(seeds[6], (N_GX, N_GY, N_GZ, NGLL * NGLL * NGLL, E_DEV), ((0, 4), (1, 8), (2, 8)), -0.2, 0.2)), 0.02, 0.1),
        "shear_mod": jnp.clip(jnp.exp(math.log(0.1) - 1.609438 * jax.random.uniform(seeds[7], (N_GX, N_GY, N_GZ, NGLL * NGLL * NGLL, E_DEV), jnp.float32) ** block_levels(seeds[7], (N_GX, N_GY, N_GZ, NGLL * NGLL * NGLL, E_DEV), ((0, 4), (1, 8), (2, 8)), -0.2, 0.2)), 0.02, 0.1),
        "density": jnp.clip(jnp.exp(math.log(3.0) - 1.0986123 * jax.random.uniform(seeds[8], (N_GX, N_GY, N_GZ, NGLL * NGLL * NGLL, E_DEV), jnp.float32) ** block_levels(seeds[8], (N_GX, N_GY, N_GZ, NGLL * NGLL * NGLL, E_DEV), ((0, 4), (1, 8), (2, 8)), -0.2, 0.2)), 1.0, 3.0),
    }


time_step = 0.1

def derivative_table():
    points = np.array([-1.0, -np.sqrt(3.0 / 7.0), 0.0, np.sqrt(3.0 / 7.0), 1.0])
    points_count = points.shape[0]
    weights = np.array([1.0 / np.prod([points[source] - points[other] for other in range(points_count) if other != source]) for source in range(points_count)])
    deriv_table = np.zeros((points_count, points_count))
    for target in range(points_count):
        for source in range(points_count):
            if target != source:
                deriv_table[target, source] = weights[source] / weights[target] / (points[target] - points[source])
        deriv_table[target, target] = -np.sum(deriv_table[target])
    return deriv_table

def element_force(position, node_index, inv_map, jac_weight, lame_first, shear_mod, deriv):
    highest = lax.Precision.HIGHEST
    elements = node_index.shape[1]
    nodes = position.shape[1]
    local = position[:, node_index].reshape(3, 5, 5, 5, elements)
    grad_a = jnp.einsum('ap,cpbke->cabke', deriv, local, precision=highest).reshape(3, 125, elements)
    grad_b = jnp.einsum('bp,capke->cabke', deriv, local, precision=highest).reshape(3, 125, elements)
    grad_c = jnp.einsum('kp,cabpe->cabke', deriv, local, precision=highest).reshape(3, 125, elements)
    mapping = inv_map.reshape(3, 3, 125, elements)
    strain_grad = grad_a[:, None] * mapping[0][None] + grad_b[:, None] * mapping[1][None] + grad_c[:, None] * mapping[2][None]
    divergence = strain_grad[0, 0] + strain_grad[1, 1] + strain_grad[2, 2]
    identity = jnp.eye(3, dtype=jnp.float32)[:, :, None, None]
    stress = shear_mod * (strain_grad + jnp.swapaxes(strain_grad, 0, 1)) + lame_first * divergence * identity
    flux = stress[:, 0][:, None] * mapping[:, 0][None] + stress[:, 1][:, None] * mapping[:, 1][None] + stress[:, 2][:, None] * mapping[:, 2][None]
    flux = (jac_weight * flux).reshape(3, 3, 5, 5, 5, elements)
    terms = jnp.einsum('pa,cpbke->cabke', deriv, flux[:, 0], precision=highest)
    terms = terms + jnp.einsum('pb,capke->cabke', deriv, flux[:, 1], precision=highest)
    terms = terms + jnp.einsum('pk,cabpe->cabke', deriv, flux[:, 2], precision=highest)
    return jnp.zeros((3, nodes), jnp.float32).at[:, node_index].add(-terms.reshape(3, 125, elements))

def fold_planes(field, dev_axis, node_axis):
    length = field.shape[node_axis]
    devices = field.shape[dev_axis]
    first = lax.slice_in_dim(field, 0, 1, axis=node_axis)
    last = lax.slice_in_dim(field, length - 1, length, axis=node_axis)
    middle = lax.slice_in_dim(field, 1, length - 1, axis=node_axis)
    zero_plane = jnp.zeros_like(lax.slice_in_dim(first, 0, 1, axis=dev_axis))
    from_lower = jnp.concatenate([zero_plane, lax.slice_in_dim(last, 0, devices - 1, axis=dev_axis)], axis=dev_axis)
    from_upper = jnp.concatenate([lax.slice_in_dim(first, 1, devices, axis=dev_axis), zero_plane], axis=dev_axis)
    return jnp.concatenate([first + from_lower, middle, last + from_upper], axis=node_axis)

def assemble_all(field):
    for dev_axis, node_axis in ((1, 4), (2, 5), (3, 6)):
        field = fold_planes(field, dev_axis, node_axis)
    return field

def reference(displ, veloc, accel, node_index, inv_map, jac_weight, lame_first, shear_mod, density):
    devices = N_GX * N_GY * N_GZ
    node_x = 4 * EX + 1
    node_y = 4 * EY + 1
    node_z = 4 * EZ + 1
    nodes = node_x * node_y * node_z
    elements = EX * EY * EZ
    deriv = jnp.asarray(derivative_table(), jnp.float32)
    index_all = node_index.reshape(devices, 125, elements)
    map_all = inv_map.reshape(devices, 9, 125, elements)
    weight_all = jac_weight.reshape(devices, 125, elements)
    lame_all = lame_first.reshape(devices, 125, elements)
    shear_all = shear_mod.reshape(devices, 125, elements)
    dens_all = density.reshape(devices, 125, elements)

    def mass_one(items):
        index, weight, dens = items
        return jnp.zeros((nodes,), jnp.float32).at[index].add(dens * weight)
    mass_local = lax.map(mass_one, (index_all, weight_all, dens_all))
    mass = assemble_all(mass_local.reshape(1, N_GX, N_GY, N_GZ, node_x, node_y, node_z))
    mass = mass.reshape(N_GX, N_GY, N_GZ, nodes)

    def force_one(items):
        position, index, mapping, weight, lame, shear = items
        return element_force(position, index, mapping, weight, lame, shear, deriv)
    half_step = 0.5 * time_step
    half_square = 0.5 * time_step * time_step
    for step in range(STEPS):
        displ = displ + time_step * veloc + half_square * accel
        veloc = veloc + half_step * accel
        moved = jnp.moveaxis(displ.reshape(3, devices, nodes), 1, 0)
        forces = lax.map(force_one, (moved, index_all, map_all, weight_all, lame_all, shear_all))
        forces = jnp.moveaxis(forces, 0, 1).reshape(3, N_GX, N_GY, N_GZ, node_x, node_y, node_z)
        forces = assemble_all(forces).reshape(3, N_GX, N_GY, N_GZ, nodes)
        accel = forces / mass[None]
        veloc = veloc + half_step * accel
    return (displ, veloc, accel)
```

```python
import functools

import jax
import jax.numpy as jnp
import numpy as np
from jax import lax
from jax.experimental import pallas as pl
from jax.experimental.pallas import tpu as pltpu
from jax.sharding import PartitionSpec as P

EX = 4
EY = 16
EZ = 2
NX = 4 * EX + 1
NY = 4 * EY + 1
NZ = 4 * EZ + 1
NODES = NX * NY * NZ
ROW = NY * NZ
XPAD = 24
FROWS = 960

time_step = 0.1
HALF = 0.5 * time_step
HALF_SQ = 0.5 * time_step * time_step
F32 = jnp.float32
BF16 = jnp.bfloat16
VMEM = pl.BlockSpec(memory_space=pltpu.VMEM)
HBM = pl.BlockSpec(memory_space=pltpu.HBM)


def derivative_table():
    points = np.array([-1.0, -np.sqrt(3.0 / 7.0), 0.0, np.sqrt(3.0 / 7.0), 1.0])
    count = points.shape[0]
    weights = np.array(
        [
            1.0 / np.prod([points[s] - points[o] for o in range(count) if o != s])
            for s in range(count)
        ]
    )
    table = np.zeros((count, count))
    for target in range(count):
        for source in range(count):
            if target != source:
                table[target, source] = (
                    weights[source] / weights[target] / (points[target] - points[source])
                )
        table[target, target] = -np.sum(table[target])
    return table


def operator_tables():
    table = derivative_table().astype(np.float32).astype(np.float64)
    eye = np.eye(5)
    full = np.zeros((3, 128, 128))
    full[0, :125, :125] = np.kron(np.kron(table, eye), eye)
    full[1, :125, :125] = np.kron(np.kron(eye, table), eye)
    full[2, :125, :125] = np.kron(np.kron(eye, eye), table)
    forward = full.reshape(384, 128)
    backward = -np.transpose(full, (2, 0, 1)).reshape(128, 384)
    out = []
    for matrix in (forward, backward):
        high = matrix.astype(np.float32).astype(jnp.bfloat16)
        low = (matrix - high.astype(np.float64)).astype(np.float32).astype(jnp.bfloat16)
        out.append(np.concatenate([high, low], axis=0))
    return out


def split(value):
    high = value.astype(BF16)
    return high, (value - high.astype(F32)).astype(BF16)


def dot(lhs, rhs):
    return lax.dot_general(lhs, rhs, (((1,), (0,)), ((), ())), preferred_element_type=F32)


def take(value, index):
    return jnp.take_along_axis(value, index, axis=1, mode="promise_in_bounds")


def lanes(shape=(8, 128)):
    return lax.broadcasted_iota(jnp.int32, shape, len(shape) - 1)


def force_kernel(
    d_hbm, v_hbm, a_hbm, n_hbm, m_hbm, j_hbm, l_hbm, s_hbm, r_hbm, fw_hbm, bw_hbm,
    t_ref, o_ref, y_ref, vh_ref, d_out,
    d_s, v_s, a_s, n_s, m_s, j_s, l_s, s_s, r_s, fw_s, bw_s,
    pos_s, grid_s, nodal_s, local_s, grad_s, fluxh_s, fluxl_s, sems,
):
    copies = []
    moves = [(d_hbm, d_s), (v_hbm, v_s), (a_hbm, a_s), (n_hbm.at[pl.ds(0, 1)], n_s), (fw_hbm, fw_s)]
    for k in range(9):
        moves.append((m_hbm.at[pl.ds(125 * k, 125), 0], m_s.at[k, pl.ds(0, 125)]))
    for src, dst in ((j_hbm, j_s), (l_hbm, l_s), (s_hbm, s_s), (r_hbm, r_s)):
        moves.append((src.at[pl.ds(0, 125), 0], dst.at[pl.ds(0, 125)]))
    moves.append((bw_hbm, bw_s))
    for at, (src, dst) in enumerate(moves):
        copy = pltpu.make_async_copy(src, dst, sems.at[at])
        copy.start()
        copies.append(copy)
    for at in range(4):
        copies[at].wait()
    accel = a_s[...]
    veloc = v_s[...]
    pos_s[...] = d_s[...] + time_step * veloc + HALF_SQ * accel
    vh_ref[...] = veloc + HALF * accel
    out_copy = pltpu.make_async_copy(pos_s, d_out, sems.at[19])
    out_copy.start()
    lane = lanes()

    corner = jnp.broadcast_to(n_s[0], (8, 128))
    elem_x = (
        (corner >= 2340).astype(jnp.int32)
        + (corner >= 4680).astype(jnp.int32)
        + (corner >= 7020).astype(jnp.int32)
    )
    rest = corner - 2340 * elem_x
    elem_y = jnp.floor((rest.astype(F32) + 0.5) * (1.0 / 36.0)).astype(jnp.int32)
    elem_z = (rest - 36 * elem_y) >> 2
    group = elem_x * 2 + elem_z
    brick = (group * 16 + elem_y).astype(F32)
    column = jnp.broadcast_to(brick[0:1], (128, 128)).T
    hit = column == lanes((128, 128)).astype(F32)
    slot_index = lax.broadcasted_iota(jnp.int32, (128, 128), 0).astype(F32)
    slot_of = jnp.sum(jnp.where(hit, slot_index, 0.0), axis=0, keepdims=True)
    slot_of = jnp.broadcast_to(slot_of, (8, 128)).astype(jnp.int32)

    for m in range(3):
        for x in range(NX):
            grid_s[m, x : x + 1, :ROW] = pos_s[m, :, pl.ds(ROW * x, ROW)]
    for m in range(3):
        for tile in range(3):
            parts = [grid_s[m, 8 * tile : 8 * tile + 8, 128 * v : 128 * v + 128] for v in range(5)]
            for z in range(NZ):
                at = 9 * lane + z
                low = at & 127
                high = at >> 7
                got = take(parts[0], low)
                for v in range(1, 5):
                    got = jnp.where(high == v, take(parts[v], low), got)
                nodal_s[m, z, 8 * tile : 8 * tile + 8, :] = got

    masks = [group == g for g in range(8)]
    indices = [4 * elem_y + b for b in range(5)]
    for m in range(3):
        local_s[m, 120:128, :] = jnp.zeros((8, 128), F32)
        for c in range(5):
            parts = [
                nodal_s[m, 4 * (g % 2) + c, 4 * (g // 2) : 4 * (g // 2) + 8, :] for g in range(8)
            ]
            for b in range(5):
                got = take(parts[0], indices[b])
                for g in range(1, 8):
                    got = jnp.where(masks[g], take(parts[g], indices[b]), got)
                local_s[m, pl.ds(5 * b + c, 5, stride=25), :] = got[:5]

    copies[4].wait()
    local = jnp.concatenate([local_s[m] for m in range(3)], axis=1)
    high, low = split(local)
    both = dot(fw_s[...], high)
    grad_s[...] = both[:384] + both[384:] + dot(fw_s[0:384, :], low)

    for at in range(5, 18):
        copies[at].wait()
    for chunk in range(8):
        at = 16 * chunk
        rows = slice(at, at + 16)
        g = [
            [grad_s[128 * l + at : 128 * l + at + 16, 128 * c : 128 * c + 128] for c in range(3)]
            for l in range(3)
        ]
        mp = [[m_s[3 * l + j, rows, :] for j in range(3)] for l in range(3)]
        gr = [
            [g[0][c] * mp[0][j] + g[1][c] * mp[1][j] + g[2][c] * mp[2][j] for j in range(3)]
            for c in range(3)
        ]
        mu = s_s[rows, :]
        trace = l_s[rows, :] * (gr[0][0] + gr[1][1] + gr[2][2])
        weight = j_s[rows, :]
        stress = [[None] * 3 for _ in range(3)]
        for c in range(3):
            for j in range(c, 3):
                value = mu * (gr[c][j] + gr[j][c])
                stress[c][j] = stress[j][c] = value + trace if c == j else value
        keep = lax.broadcasted_iota(jnp.int32, (16, 128), 0) < 125 - at
        mass = r_s[rows, :] * weight
        t_ref[3, rows, :] = jnp.where(keep, mass, 0.0) if chunk == 7 else mass
        for l in range(3):
            for c in range(3):
                flux = weight * (
                    stress[c][0] * mp[l][0] + stress[c][1] * mp[l][1] + stress[c][2] * mp[l][2]
                )
                if chunk == 7:
                    flux = jnp.where(keep, flux, 0.0)
                high, low = split(flux)
                to = slice(128 * l + at, 128 * l + at + 16)
                cols = slice(128 * c, 128 * c + 128)
                fluxh_s[to, cols] = high
                fluxl_s[to, cols] = low

    copies[18].wait()
    both = dot(bw_s[...], fluxh_s[...])
    terms = both[:128] + both[128:] + dot(bw_s[0:128, :], fluxl_s[...])
    for m in range(3):
        t_ref[m, 0:128, :] = terms[:, 128 * m : 128 * m + 128]
    for m in range(4):
        t_ref[m, 128:200, :] = jnp.zeros((72, 128), F32)
    o_ref[...] = slot_of

    edge = take(slot_of, 16 * (lane & 7) + 15 * ((lane >> 3) & 1))
    second = ((lane >> 3) & 1) == 1
    packs = []
    for q in range(3):
        pack = jnp.zeros((8, 128), F32)
        for k in range(8 * q, min(8 * q + 8, 20)):
            m, c = divmod(k, 5)
            got = jnp.where(
                second,
                take(t_ref[m, pl.ds(20 + c, 8, stride=25), :], edge),
                take(t_ref[m, pl.ds(c, 8, stride=25), :], edge),
            )
            pack = jnp.where((lane >> 4) == k - 8 * q, got, pack)
        packs.append(pack)
    even = 1 - lax.axis_index("gy") % 2
    upper = (lane >= 64).astype(jnp.int32)
    face = upper + even - 2 * upper * even
    plane = lane - 64 * upper
    comp = (
        (plane >= 9).astype(jnp.int32)
        + (plane >= 18).astype(jnp.int32)
        + (plane >= 27).astype(jnp.int32)
    )
    z = plane - 9 * comp
    row = lax.broadcasted_iota(jnp.int32, (8, 128), 0)
    zero = jnp.zeros((8, 128), F32)
    parts = []
    for x in range(4):
        total = zero
        for h in range(2):
            c = z - 4 * h
            good = (c >= 0) & (c <= 4) & (plane < 36)
            k = 5 * comp + c
            at = (16 * (k & 7) + 8 * face + 2 * x + h) & 127
            for q in range(3):
                total = total + jnp.where(good & ((k >> 3) == q), take(packs[q], at), zero)
        parts.append(total)
    stack_rows(parts, row, zero, y_ref, 0)
    out_copy.wait()


def stack_rows(parts, row, zero, out_ref, at):
    second = pltpu.roll(parts[1], 4, 0)
    fourth = pltpu.roll(parts[3], 4, 0)
    out_ref[at : at + 8, :] = parts[0] + jnp.where(row >= 4, second, zero)
    out_ref[at + 8 : at + 16, :] = (
        parts[2] + jnp.where(row < 4, second, zero) + jnp.where(row >= 4, fourth, zero)
    )
    out_ref[at + 16 : at + 24, :] = jnp.where(row < 4, fourth, zero)


def field_kernel(t_ref, o_ref, f_ref):
    slot_of = o_ref[...]
    lane = lanes()
    gathers = []
    for g in range(8):
        base = 16 * g + (lane >> 2)
        gathers.append(
            (take(slot_of, jnp.minimum(base, 127)), take(slot_of, jnp.clip(base - 1, 0, 127)))
        )
    quarter = lane & 3
    inside = lane < 64
    firsts = [(quarter == b) & inside for b in range(4)]
    lasts = (quarter == 0) & (lane >= 4) & (lane < 68)
    row = lax.broadcasted_iota(jnp.int32, (8, 128), 0)
    zero = jnp.zeros((8, 128), F32)
    for m in range(4):
        planes = {}
        for c in range(5):
            parts = [t_ref[m, pl.ds(5 * b + c, 8, stride=25), :] for b in range(5)]
            for g in range(8):
                at, before = gathers[g]
                got = jnp.where(firsts[0], take(parts[0], at), zero)
                for b in range(1, 4):
                    got = jnp.where(firsts[b], take(parts[b], at), got)
                got = got + jnp.where(lasts, take(parts[4], before), zero)
                key = (4 * (g % 2) + c, g // 2)
                planes[key] = planes[key] + got if key in planes else got
        for z in range(NZ):
            stack_rows([planes[(z, x)] for x in range(4)], row, zero, f_ref, (m * 9 + z) * XPAD)
    f_ref[36 * XPAD : FROWS, :] = jnp.zeros((FROWS - 36 * XPAD, 128), F32)


def y_faces(ya, yb):
    at = lax.axis_index("gy")
    odd = at % 2 == 1
    outer = (at > 0) & (at < lax.axis_size("gy") - 1)
    far = jnp.where(outer, yb, 0.0)
    return jnp.where(odd, ya, far), jnp.where(odd, far, ya)


def x_kernel(ya_ref, yb_ref, f_ref, xa_ref, xb_ref):
    pad = jnp.zeros((128 - XPAD, 128), F32)
    near = jnp.concatenate([ya_ref[...], pad], axis=0).T[0:40]
    far = jnp.concatenate([yb_ref[...], pad], axis=0).T[64:104]
    lo, hi = y_faces(near, far)
    lane = lanes((40, 128))

    def face(x):
        return (
            f_ref[pl.ds(x, 40, stride=XPAD), :]
            + jnp.where(lane == 0, pltpu.roll(lo, (128 - x) % 128, 1) if x else lo, 0.0)
            + jnp.where(lane == 64, pltpu.roll(hi, 64 - x, 1), 0.0)
        )

    first = face(0)
    last = face(16)
    odd = lax.axis_index("gx") % 2 == 1
    xa_ref[...] = jnp.where(odd, first, last)
    xb_ref[...] = jnp.where(odd, last, first)


def y_kernel(ya_ref, yb_ref, f_in, f_ref):
    lane = lanes()
    for tile in range(3):
        rows = slice(8 * tile, 8 * tile + 8)
        lo, hi = y_faces(ya_ref[rows, :], pltpu.roll(yb_ref[rows, :], 64, 1))
        for plane in range(36):
            to = slice(plane * XPAD + 8 * tile, plane * XPAD + 8 * tile + 8)
            low = pltpu.roll(lo, 128 - plane, 1) if plane else lo
            f_ref[to, :] = (
                f_in[to, :]
                + jnp.where(lane == 0, low, 0.0)
                + jnp.where(lane == 64, pltpu.roll(hi, (64 - plane) % 128, 1), 0.0)
            )


def z_kernel(xa_ref, xb_ref, f_in, f_ref, za_ref, zb_ref):
    at = lax.axis_index("gx")
    odd = at % 2 == 1
    outer = (at > 0) & (at < lax.axis_size("gx") - 1)
    near = xa_ref[0:36, :]
    far = jnp.where(outer, xb_ref[0:36, :], 0.0)
    f_ref[0 : 36 * XPAD, :] = f_in[0 : 36 * XPAD, :]
    f_ref[pl.ds(0, 36, stride=XPAD), :] = f_in[pl.ds(0, 36, stride=XPAD), :] + jnp.where(
        odd, near, far
    )
    f_ref[pl.ds(16, 36, stride=XPAD), :] = f_in[pl.ds(16, 36, stride=XPAD), :] + jnp.where(
        odd, far, near
    )
    odd = lax.axis_index("gz") % 2 == 1
    for m in range(4):
        at = m * 9 * XPAD
        first = f_ref[at : at + XPAD, :]
        last = f_ref[at + 8 * XPAD : at + 9 * XPAD, :]
        za_ref[XPAD * m : XPAD * m + XPAD, :] = jnp.where(odd, first, last)
        zb_ref[XPAD * m : XPAD * m + XPAD, :] = jnp.where(odd, last, first)


def end_kernel(za_ref, zb_ref, f_ref, vh_ref, v_out, a_out, a_s, v_s, acc_s, grid_s, sems):
    at = lax.axis_index("gz")
    odd = at % 2 == 1
    outer = (at > 0) & (at < lax.axis_size("gz") - 1)
    lane = lanes()

    def added(m, z, tile):
        value = f_ref[(m * 9 + z) * XPAD + 8 * tile : (m * 9 + z) * XPAD + 8 * tile + 8, :]
        if z in (0, 8):
            rows = slice(XPAD * m + 8 * tile, XPAD * m + 8 * tile + 8)
            near = za_ref[rows, :]
            far = jnp.where(outer, zb_ref[rows, :], 0.0)
            value = value + (jnp.where(odd, near, far) if z == 0 else jnp.where(odd, far, near))
        return value

    for z in range(NZ):
        for tile in range(3):
            mass = added(3, z, tile)
            for m in range(3):
                acc_s[m, z, 8 * tile : 8 * tile + 8, :] = added(m, z, tile) / mass
    for m in range(3):
        for tile in range(3):
            parts = [acc_s[m, z, 8 * tile : 8 * tile + 8, :] for z in range(NZ)]
            for v in range(5):
                at = lane + 128 * v
                y = jnp.floor((at.astype(F32) + 0.5) * (1.0 / 9.0)).astype(jnp.int32)
                z_of = at - 9 * y
                got = take(parts[0], y)
                for z in range(1, NZ):
                    got = jnp.where(z_of == z, take(parts[z], y), got)
                grid_s[m, 8 * tile : 8 * tile + 8, 128 * v : 128 * v + 128] = got
    for m in range(3):
        for x in range(NX):
            a_s[m, :, pl.ds(ROW * x, ROW)] = grid_s[m, x : x + 1, :ROW]
    a_copy = pltpu.make_async_copy(a_s, a_out, sems.at[0])
    a_copy.start()
    v_s[...] = vh_ref[...] + HALF * a_s[...]
    v_copy = pltpu.make_async_copy(v_s, v_out, sems.at[1])
    v_copy.start()
    a_copy.wait()
    v_copy.wait()


def swap(value, at, second):
    axes = ("gx", "gy", "gz")
    sizes = [lax.axis_size(axis) for axis in axes]
    other = 0 if at == 2 else 2
    pairs = []
    for index in np.ndindex(*sizes):
        target = list(index)
        if not second:
            target[at] ^= 1
        elif 0 < index[at] < sizes[at] - 1:
            target[at] = ((index[at] - 1) ^ 1) + 1
        else:
            target[other] ^= 1
        pairs.append(tuple(int(np.ravel_multi_index(i, sizes)) for i in (index, target)))
    return lax.ppermute(value, axes, pairs)


def body(displ, veloc, accel, node_index, inv_map, jac_weight, lame_first, shear_mod, density):
    f32 = functools.partial(jax.ShapeDtypeStruct, dtype=F32)
    flat = (3, 1, NODES)
    points = (125, 1, 128)
    tables = [jnp.asarray(table) for table in operator_tables()]
    scratch = [
        pltpu.VMEM(flat, F32), pltpu.VMEM(flat, F32), pltpu.VMEM(flat, F32),
        pltpu.VMEM((1, 1, 128), jnp.int32),
        pltpu.VMEM((9, 128, 128), F32),
        pltpu.VMEM((128, 128), F32), pltpu.VMEM((128, 128), F32),
        pltpu.VMEM((128, 128), F32), pltpu.VMEM((128, 128), F32),
        pltpu.VMEM((768, 128), BF16), pltpu.VMEM((256, 384), BF16),
        pltpu.VMEM(flat, F32), pltpu.VMEM((3, 24, 640), F32), pltpu.VMEM((3, 9, 24, 128), F32),
        pltpu.VMEM((3, 128, 128), F32), pltpu.VMEM((384, 384), F32),
        pltpu.VMEM((384, 384), BF16), pltpu.VMEM((384, 384), BF16),
        pltpu.SemaphoreType.DMA((20,)),
    ]
    terms, slots, ya, v_half, displ_out = pl.pallas_call(
        force_kernel,
        out_shape=(
            f32((4, 200, 128)), jax.ShapeDtypeStruct((8, 128), jnp.int32), f32((XPAD, 128)),
            f32(flat), f32(flat),
        ),
        in_specs=[HBM] * 11,
        out_specs=(VMEM, VMEM, VMEM, VMEM, HBM),
        scratch_shapes=scratch,
        compiler_params=pltpu.CompilerParams(vmem_limit_bytes=16 << 20),
    )(
        *(
            pltpu.with_memory_space_constraint(value, pltpu.HBM)
            for value in (
                displ.reshape(flat), veloc.reshape(flat), accel.reshape(flat),
                node_index.reshape(points), inv_map.reshape(1125, 1, 128),
                jac_weight.reshape(points), lame_first.reshape(points), shear_mod.reshape(points),
                density.reshape(points), *tables,
            )
        )
    )
    small = pltpu.CompilerParams(vmem_limit_bytes=8 << 20)
    ya = swap(ya, 1, False)
    field = pl.pallas_call(
        field_kernel,
        out_shape=f32((FROWS, 128)),
        in_specs=[VMEM] * 2,
        out_specs=VMEM,
        compiler_params=small,
        cost_estimate=pl.CostEstimate(flops=4000000, bytes_accessed=800000, transcendentals=0),
    )(terms, slots)
    count = lax.axis_size("gy")
    hops = [(i, (i + 2) % count if i % 2 == 0 else (i - 2) % count) for i in range(count)]
    yb = lax.ppermute(ya, "gy", hops)
    face = f32((40, 128))
    xa, xb = pl.pallas_call(
        x_kernel,
        out_shape=(face, face),
        in_specs=[VMEM] * 3,
        out_specs=(VMEM,) * 2,
        compiler_params=small,
    )(ya, yb, field)
    field = pl.pallas_call(
        y_kernel,
        out_shape=f32((FROWS, 128)),
        in_specs=[VMEM] * 3,
        out_specs=VMEM,
        input_output_aliases={2: 0},
        compiler_params=small,
        cost_estimate=pl.CostEstimate(flops=1000000, bytes_accessed=800000, transcendentals=0),
    )(ya, yb, field)
    xa = swap(xa, 0, False)
    xb = swap(xb, 0, True)
    face = f32((96, 128))
    field, za, zb = pl.pallas_call(
        z_kernel,
        out_shape=(f32((FROWS, 128)), face, face),
        in_specs=[VMEM] * 3,
        out_specs=(VMEM,) * 3,
        input_output_aliases={2: 0},
        compiler_params=pltpu.CompilerParams(vmem_limit_bytes=8 << 20),
    )(xa, xb, field)
    za = swap(za, 2, False)
    zb = swap(zb, 2, True)
    veloc_out, accel_out = pl.pallas_call(
        end_kernel,
        out_shape=(f32(flat), f32(flat)),
        in_specs=[VMEM] * 4,
        out_specs=(HBM, HBM),
        scratch_shapes=[
            pltpu.VMEM(flat, F32), pltpu.VMEM(flat, F32), pltpu.VMEM((3, 9, 24, 128), F32),
            pltpu.VMEM((3, 24, 640), F32), pltpu.SemaphoreType.DMA((2,)),
        ],
        compiler_params=pltpu.CompilerParams(vmem_limit_bytes=8 << 20),
    )(za, zb, field, v_half)
    shape = (3, 1, 1, 1, NODES)
    return displ_out.reshape(shape), veloc_out.reshape(shape), accel_out.reshape(shape)


def solution(mesh):
    nodal = P(None, "gx", "gy", "gz", None)
    point = P("gx", "gy", "gz", None, None)
    placed = (nodal,) * 3 + (point, P("gx", "gy", "gz", None, None, None)) + (point,) * 4
    return jax.shard_map(
        body, mesh=mesh, in_specs=placed, out_specs=(nodal,) * 3, check_vma=False
    )
```

```python
import functools

import jax
import jax.numpy as jnp
import numpy as np
from jax import lax
from jax.experimental import pallas as pl
from jax.experimental.pallas import tpu as pltpu
from jax.sharding import PartitionSpec as P

EX = 4
EY = 16
EZ = 2
NX = 4 * EX + 1
NY = 4 * EY + 1
NZ = 4 * EZ + 1
NODES = NX * NY * NZ
ROW = NY * NZ
XPAD = 24
FROWS = 960

time_step = 0.1
HALF = 0.5 * time_step
HALF_SQ = 0.5 * time_step * time_step
F32 = jnp.float32
BF16 = jnp.bfloat16
VMEM = pl.BlockSpec(memory_space=pltpu.VMEM)
HBM = pl.BlockSpec(memory_space=pltpu.HBM)


def derivative_table():
    points = np.array([-1.0, -np.sqrt(3.0 / 7.0), 0.0, np.sqrt(3.0 / 7.0), 1.0])
    count = points.shape[0]
    weights = np.array(
        [
            1.0 / np.prod([points[s] - points[o] for o in range(count) if o != s])
            for s in range(count)
        ]
    )
    table = np.zeros((count, count))
    for target in range(count):
        for source in range(count):
            if target != source:
                table[target, source] = (
                    weights[source] / weights[target] / (points[target] - points[source])
                )
        table[target, target] = -np.sum(table[target])
    return table


def operator_tables():
    table = derivative_table().astype(np.float32).astype(np.float64)
    eye = np.eye(5)
    full = np.zeros((3, 128, 128))
    full[0, :125, :125] = np.kron(np.kron(table, eye), eye)
    full[1, :125, :125] = np.kron(np.kron(eye, table), eye)
    full[2, :125, :125] = np.kron(np.kron(eye, eye), table)
    forward = full.reshape(384, 128)
    backward = -np.transpose(full, (2, 0, 1)).reshape(128, 384)
    out = []
    for matrix in (forward, backward):
        high = matrix.astype(np.float32).astype(jnp.bfloat16)
        low = (matrix - high.astype(np.float64)).astype(np.float32).astype(jnp.bfloat16)
        out.append(np.concatenate([high, low], axis=0))
    return out


def split(value):
    high = value.astype(BF16)
    return high, (value - high.astype(F32)).astype(BF16)


def dot(lhs, rhs):
    return lax.dot_general(lhs, rhs, (((1,), (0,)), ((), ())), preferred_element_type=F32)


def take(value, index):
    return jnp.take_along_axis(value, index, axis=1, mode="promise_in_bounds")


def lanes(shape=(8, 128)):
    return lax.broadcasted_iota(jnp.int32, shape, len(shape) - 1)


def force_kernel(
    d_hbm, v_hbm, a_hbm, n_hbm, m_hbm, j_hbm, l_hbm, s_hbm, r_hbm, fw_hbm, bw_hbm,
    t_ref, o_ref, y_ref, vh_ref, d_out,
    d_s, v_s, a_s, n_s, m_s, j_s, l_s, s_s, r_s, fw_s, bw_s,
    pos_s, grid_s, nodal_s, local_s, grad_s, fluxh_s, fluxl_s, sems,
):
    copies = []
    moves = [(d_hbm, d_s), (v_hbm, v_s), (a_hbm, a_s), (n_hbm.at[pl.ds(0, 1)], n_s), (fw_hbm, fw_s)]
    for k in range(9):
        moves.append((m_hbm.at[pl.ds(125 * k, 125), 0], m_s.at[k, pl.ds(0, 125)]))
    for src, dst in ((j_hbm, j_s), (l_hbm, l_s), (s_hbm, s_s), (r_hbm, r_s)):
        moves.append((src.at[pl.ds(0, 125), 0], dst.at[pl.ds(0, 125)]))
    moves.append((bw_hbm, bw_s))
    for at, (src, dst) in enumerate(moves):
        copy = pltpu.make_async_copy(src, dst, sems.at[at])
        copy.start()
        copies.append(copy)
    for at in range(4):
        copies[at].wait()
    accel = a_s[...]
    veloc = v_s[...]
    pos_s[...] = d_s[...] + time_step * veloc + HALF_SQ * accel
    vh_ref[...] = veloc + HALF * accel
    out_copy = pltpu.make_async_copy(pos_s, d_out, sems.at[19])
    out_copy.start()
    lane = lanes()

    corner = jnp.broadcast_to(n_s[0], (8, 128))
    elem_x = (
        (corner >= 2340).astype(jnp.int32)
        + (corner >= 4680).astype(jnp.int32)
        + (corner >= 7020).astype(jnp.int32)
    )
    rest = corner - 2340 * elem_x
    elem_y = jnp.floor((rest.astype(F32) + 0.5) * (1.0 / 36.0)).astype(jnp.int32)
    elem_z = (rest - 36 * elem_y) >> 2
    group = elem_x * 2 + elem_z
    brick = (group * 16 + elem_y).astype(F32)
    column = jnp.broadcast_to(brick[0:1], (128, 128)).T
    hit = column == lanes((128, 128)).astype(F32)
    slot_index = lax.broadcasted_iota(jnp.int32, (128, 128), 0).astype(F32)
    slot_of = jnp.sum(jnp.where(hit, slot_index, 0.0), axis=0, keepdims=True)
    slot_of = jnp.broadcast_to(slot_of, (8, 128)).astype(jnp.int32)

    for m in range(3):
        for x in range(NX):
            value = pos_s[m, :, pl.ds(ROW * x, ROW)]
            if x < 16:
                grid_s[m, x : x + 1, :ROW] = value
            else:
                grid_s[3, m : m + 1, :ROW] = value
    places = [9 * (lane & 63) + 4 * (lane >> 6) + c for c in range(5)]
    for u in range(2):
        c = jnp.minimum(4 * u + (lane >> 5), 4)
        places.append(36 * (lane & 15) + 36 + c + 4 * ((lane >> 4) & 1))
    for m in range(4):
        for tile in range(2 if m < 3 else 1):
            rows = slice(8 * tile, 8 * tile + 8)
            parts = [grid_s[m, rows, 128 * v : 128 * v + 128] for v in range(5)]
            for c in range(7):
                low = places[c] & 127
                high = places[c] >> 7
                got = take(parts[0], low)
                for v in range(1, 5):
                    got = jnp.where(high == v, take(parts[v], low), got)
                if m < 3:
                    nodal_s[m, c, rows, :] = got
                else:
                    for k in range(3):
                        nodal_s[k, c, 16:17, :] = got[k : k + 1]

    masks = [elem_x == x for x in range(4)]
    inner = 64 * elem_z + 4 * elem_y
    outer = 16 * elem_z + elem_y
    for m in range(3):
        local_s[m, 120:128, :] = jnp.zeros((8, 128), F32)
        for c in range(5):
            near = [nodal_s[m, c, 4 * x : 4 * x + 8, :] for x in range(4)]
            last = [nodal_s[m, 5 + c // 4, 4 * x : 4 * x + 8, :] for x in range(4)]
            for b in range(5):
                parts, at = (near, inner + b) if b < 4 else (last, outer + 32 * (c % 4))
                got = take(parts[0], at)
                for x in range(1, 4):
                    got = jnp.where(masks[x], take(parts[x], at), got)
                local_s[m, pl.ds(5 * b + c, 5, stride=25), :] = got[:5]

    copies[4].wait()
    local = jnp.concatenate([local_s[m] for m in range(3)], axis=1)
    high, low = split(local)
    both = dot(fw_s[...], high)
    grad_s[...] = both[:384] + both[384:] + dot(fw_s[0:384, :], low)

    for at in range(5, 18):
        copies[at].wait()
    for chunk in range(8):
        at = 16 * chunk
        rows = slice(at, at + 16)
        g = [
            [grad_s[128 * l + at : 128 * l + at + 16, 128 * c : 128 * c + 128] for c in range(3)]
            for l in range(3)
        ]
        mp = [[m_s[3 * l + j, rows, :] for j in range(3)] for l in range(3)]
        gr = [
            [g[0][c] * mp[0][j] + g[1][c] * mp[1][j] + g[2][c] * mp[2][j] for j in range(3)]
            for c in range(3)
        ]
        mu = s_s[rows, :]
        trace = l_s[rows, :] * (gr[0][0] + gr[1][1] + gr[2][2])
        weight = j_s[rows, :]
        stress = [[None] * 3 for _ in range(3)]
        for c in range(3):
            for j in range(c, 3):
                value = mu * (gr[c][j] + gr[j][c])
                stress[c][j] = stress[j][c] = value + trace if c == j else value
        keep = lax.broadcasted_iota(jnp.int32, (16, 128), 0) < 125 - at
        mass = r_s[rows, :] * weight
        t_ref[3, rows, :] = jnp.where(keep, mass, 0.0) if chunk == 7 else mass
        for l in range(3):
            for c in range(3):
                flux = weight * (
                    stress[c][0] * mp[l][0] + stress[c][1] * mp[l][1] + stress[c][2] * mp[l][2]
                )
                if chunk == 7:
                    flux = jnp.where(keep, flux, 0.0)
                high, low = split(flux)
                to = slice(128 * l + at, 128 * l + at + 16)
                cols = slice(128 * c, 128 * c + 128)
                fluxh_s[to, cols] = high
                fluxl_s[to, cols] = low

    copies[18].wait()
    both = dot(bw_s[...], fluxh_s[...])
    terms = both[:128] + both[128:] + dot(bw_s[0:128, :], fluxl_s[...])
    for m in range(3):
        t_ref[m, 0:128, :] = terms[:, 128 * m : 128 * m + 128]
    for m in range(4):
        t_ref[m, 128:200, :] = jnp.zeros((72, 128), F32)
    o_ref[...] = slot_of

    edge = take(slot_of, 16 * (lane & 7) + 15 * ((lane >> 3) & 1))
    second = ((lane >> 3) & 1) == 1
    packs = []
    for q in range(3):
        pack = jnp.zeros((8, 128), F32)
        for k in range(8 * q, min(8 * q + 8, 20)):
            m, c = divmod(k, 5)
            got = jnp.where(
                second,
                take(t_ref[m, pl.ds(20 + c, 8, stride=25), :], edge),
                take(t_ref[m, pl.ds(c, 8, stride=25), :], edge),
            )
            pack = jnp.where((lane >> 4) == k - 8 * q, got, pack)
        packs.append(pack)
    even = 1 - lax.axis_index("gy") % 2
    upper = (lane >= 64).astype(jnp.int32)
    face = upper + even - 2 * upper * even
    plane = lane - 64 * upper
    comp = (
        (plane >= 9).astype(jnp.int32)
        + (plane >= 18).astype(jnp.int32)
        + (plane >= 27).astype(jnp.int32)
    )
    z = plane - 9 * comp
    row = lax.broadcasted_iota(jnp.int32, (8, 128), 0)
    zero = jnp.zeros((8, 128), F32)
    parts = []
    for x in range(4):
        total = zero
        for h in range(2):
            c = z - 4 * h
            good = (c >= 0) & (c <= 4) & (plane < 36)
            k = 5 * comp + c
            at = (16 * (k & 7) + 8 * face + 2 * x + h) & 127
            for q in range(3):
                total = total + jnp.where(good & ((k >> 3) == q), take(packs[q], at), zero)
        parts.append(total)
    stack_rows(parts, row, zero, y_ref, 0)
    out_copy.wait()


def stack_rows(parts, row, zero, out_ref, at):
    second = pltpu.roll(parts[1], 4, 0)
    fourth = pltpu.roll(parts[3], 4, 0)
    out_ref[at : at + 8, :] = parts[0] + jnp.where(row >= 4, second, zero)
    out_ref[at + 8 : at + 16, :] = (
        parts[2] + jnp.where(row < 4, second, zero) + jnp.where(row >= 4, fourth, zero)
    )
    out_ref[at + 16 : at + 24, :] = jnp.where(row < 4, fourth, zero)


def field_kernel(t_ref, o_ref, f_ref):
    slot_of = o_ref[...]
    lane = lanes()
    gathers = []
    for g in range(8):
        base = 16 * g + (lane >> 2)
        gathers.append(
            (take(slot_of, jnp.minimum(base, 127)), take(slot_of, jnp.clip(base - 1, 0, 127)))
        )
    quarter = lane & 3
    inside = lane < 64
    firsts = [(quarter == b) & inside for b in range(4)]
    lasts = (quarter == 0) & (lane >= 4) & (lane < 68)
    row = lax.broadcasted_iota(jnp.int32, (8, 128), 0)
    zero = jnp.zeros((8, 128), F32)
    for m in range(4):
        planes = {}
        for c in range(5):
            parts = [t_ref[m, pl.ds(5 * b + c, 8, stride=25), :] for b in range(5)]
            for g in range(8):
                at, before = gathers[g]
                got = jnp.where(firsts[0], take(parts[0], at), zero)
                for b in range(1, 4):
                    got = jnp.where(firsts[b], take(parts[b], at), got)
                got = got + jnp.where(lasts, take(parts[4], before), zero)
                key = (4 * (g % 2) + c, g // 2)
                planes[key] = planes[key] + got if key in planes else got
        for z in range(NZ):
            stack_rows([planes[(z, x)] for x in range(4)], row, zero, f_ref, (m * 9 + z) * XPAD)
    f_ref[36 * XPAD : FROWS, :] = jnp.zeros((FROWS - 36 * XPAD, 128), F32)


def y_faces(ya, yb):
    at = lax.axis_index("gy")
    odd = at % 2 == 1
    outer = (at > 0) & (at < lax.axis_size("gy") - 1)
    far = jnp.where(outer, yb, 0.0)
    return jnp.where(odd, ya, far), jnp.where(odd, far, ya)


def x_kernel(ya_ref, yb_ref, f_ref, xa_ref, xb_ref):
    pad = jnp.zeros((128 - XPAD, 128), F32)
    near = jnp.concatenate([ya_ref[...], pad], axis=0).T[0:40]
    far = jnp.concatenate([yb_ref[...], pad], axis=0).T[64:104]
    lo, hi = y_faces(near, far)
    lane = lanes((40, 128))

    def face(x):
        return (
            f_ref[pl.ds(x, 40, stride=XPAD), :]
            + jnp.where(lane == 0, pltpu.roll(lo, (128 - x) % 128, 1) if x else lo, 0.0)
            + jnp.where(lane == 64, pltpu.roll(hi, 64 - x, 1), 0.0)
        )

    first = face(0)
    last = face(16)
    odd = lax.axis_index("gx") % 2 == 1
    xa_ref[...] = jnp.where(odd, first, last)
    xb_ref[...] = jnp.where(odd, last, first)


def y_kernel(ya_ref, yb_ref, f_in, f_ref):
    lane = lanes()
    for tile in range(3):
        rows = slice(8 * tile, 8 * tile + 8)
        lo, hi = y_faces(ya_ref[rows, :], pltpu.roll(yb_ref[rows, :], 64, 1))
        for plane in range(36):
            to = slice(plane * XPAD + 8 * tile, plane * XPAD + 8 * tile + 8)
            low = pltpu.roll(lo, 128 - plane, 1) if plane else lo
            f_ref[to, :] = (
                f_in[to, :]
                + jnp.where(lane == 0, low, 0.0)
                + jnp.where(lane == 64, pltpu.roll(hi, (64 - plane) % 128, 1), 0.0)
            )


def z_kernel(xa_ref, xb_ref, f_in, f_ref, za_ref, zb_ref):
    at = lax.axis_index("gx")
    odd = at % 2 == 1
    outer = (at > 0) & (at < lax.axis_size("gx") - 1)
    near = xa_ref[0:36, :]
    far = jnp.where(outer, xb_ref[0:36, :], 0.0)
    f_ref[0 : 36 * XPAD, :] = f_in[0 : 36 * XPAD, :]
    f_ref[pl.ds(0, 36, stride=XPAD), :] = f_in[pl.ds(0, 36, stride=XPAD), :] + jnp.where(
        odd, near, far
    )
    f_ref[pl.ds(16, 36, stride=XPAD), :] = f_in[pl.ds(16, 36, stride=XPAD), :] + jnp.where(
        odd, far, near
    )
    odd = lax.axis_index("gz") % 2 == 1
    for m in range(4):
        at = m * 9 * XPAD
        first = f_ref[at : at + XPAD, :]
        last = f_ref[at + 8 * XPAD : at + 9 * XPAD, :]
        za_ref[XPAD * m : XPAD * m + XPAD, :] = jnp.where(odd, first, last)
        zb_ref[XPAD * m : XPAD * m + XPAD, :] = jnp.where(odd, last, first)


def end_kernel(za_ref, zb_ref, f_ref, vh_ref, v_out, a_out, a_s, v_s, acc_s, grid_s, sems):
    at = lax.axis_index("gz")
    odd = at % 2 == 1
    outer = (at > 0) & (at < lax.axis_size("gz") - 1)
    lane = lanes()
    spots = []
    for v in range(5):
        at = lane + 128 * v
        y = jnp.floor((at.astype(F32) + 0.5) * (1.0 / 9.0)).astype(jnp.int32)
        spots.append((y, at - 9 * y))

    def added(m, z, tile):
        value = f_ref[(m * 9 + z) * XPAD + 8 * tile : (m * 9 + z) * XPAD + 8 * tile + 8, :]
        if z in (0, 8):
            rows = slice(XPAD * m + 8 * tile, XPAD * m + 8 * tile + 8)
            near = za_ref[rows, :]
            far = jnp.where(outer, zb_ref[rows, :], 0.0)
            value = value + (jnp.where(odd, near, far) if z == 0 else jnp.where(odd, far, near))
        return value

    def to_rows(m, tile):
        rows = slice(8 * tile, 8 * tile + 8)
        parts = [acc_s[m, z, rows, :] for z in range(NZ)]
        for v in range(5):
            y, z_of = spots[v]
            got = take(parts[0], y)
            for z in range(1, NZ):
                got = jnp.where(z_of == z, take(parts[z], y), got)
            grid_s[m, rows, 128 * v : 128 * v + 128] = got

    for z in range(NZ):
        for tile in range(3):
            mass = added(3, z, tile)
            for m in range(3):
                value = added(m, z, tile) / mass
                if tile < 2:
                    acc_s[m, z, 8 * tile : 8 * tile + 8, :] = value
                else:
                    acc_s[3, z, m : m + 1, :] = value[0:1]
    to_rows(3, 0)
    copies = []
    for m in range(3):
        to_rows(m, 0)
        to_rows(m, 1)
        for x in range(16):
            a_s[m, :, pl.ds(ROW * x, ROW)] = grid_s[m, x : x + 1, :ROW]
        a_s[m, :, pl.ds(ROW * 16, ROW)] = grid_s[3, m : m + 1, :ROW]
        v_s[m] = vh_ref[m] + HALF * a_s[m]
        for k, (src, dst) in enumerate(((a_s, a_out), (v_s, v_out))):
            copy = pltpu.make_async_copy(src.at[m], dst.at[m], sems.at[2 * m + k])
            copy.start()
            copies.append(copy)
    for copy in copies:
        copy.wait()


def swap(value, at, second):
    axes = ("gx", "gy", "gz")
    sizes = [lax.axis_size(axis) for axis in axes]
    other = 0 if at == 2 else 2
    pairs = []
    for index in np.ndindex(*sizes):
        target = list(index)
        if not second:
            target[at] ^= 1
        elif 0 < index[at] < sizes[at] - 1:
            target[at] = ((index[at] - 1) ^ 1) + 1
        else:
            target[other] ^= 1
        pairs.append(tuple(int(np.ravel_multi_index(i, sizes)) for i in (index, target)))
    return lax.ppermute(value, axes, pairs)


def body(displ, veloc, accel, node_index, inv_map, jac_weight, lame_first, shear_mod, density):
    f32 = functools.partial(jax.ShapeDtypeStruct, dtype=F32)
    flat = (3, 1, NODES)
    points = (125, 1, 128)
    tables = [jnp.asarray(table) for table in operator_tables()]
    scratch = [
        pltpu.VMEM(flat, F32), pltpu.VMEM(flat, F32), pltpu.VMEM(flat, F32),
        pltpu.VMEM((1, 1, 128), jnp.int32),
        pltpu.VMEM((9, 128, 128), F32),
        pltpu.VMEM((128, 128), F32), pltpu.VMEM((128, 128), F32),
        pltpu.VMEM((128, 128), F32), pltpu.VMEM((128, 128), F32),
        pltpu.VMEM((768, 128), BF16), pltpu.VMEM((256, 384), BF16),
        pltpu.VMEM(flat, F32), pltpu.VMEM((4, 16, 640), F32), pltpu.VMEM((3, 7, 24, 128), F32),
        pltpu.VMEM((3, 128, 128), F32), pltpu.VMEM((384, 384), F32),
        pltpu.VMEM((384, 384), BF16), pltpu.VMEM((384, 384), BF16),
        pltpu.SemaphoreType.DMA((20,)),
    ]
    terms, slots, ya, v_half, displ_out = pl.pallas_call(
        force_kernel,
        out_shape=(
            f32((4, 200, 128)), jax.ShapeDtypeStruct((8, 128), jnp.int32), f32((XPAD, 128)),
            f32(flat), f32(flat),
        ),
        in_specs=[HBM] * 11,
        out_specs=(VMEM, VMEM, VMEM, VMEM, HBM),
        scratch_shapes=scratch,
        compiler_params=pltpu.CompilerParams(vmem_limit_bytes=16 << 20),
    )(
        *(
            pltpu.with_memory_space_constraint(value, pltpu.HBM)
            for value in (
                displ.reshape(flat), veloc.reshape(flat), accel.reshape(flat),
                node_index.reshape(points), inv_map.reshape(1125, 1, 128),
                jac_weight.reshape(points), lame_first.reshape(points), shear_mod.reshape(points),
                density.reshape(points), *tables,
            )
        )
    )
    small = pltpu.CompilerParams(vmem_limit_bytes=8 << 20)
    ya = swap(ya, 1, False)
    field = pl.pallas_call(
        field_kernel,
        out_shape=f32((FROWS, 128)),
        in_specs=[VMEM] * 2,
        out_specs=VMEM,
        compiler_params=small,
        cost_estimate=pl.CostEstimate(flops=4000000, bytes_accessed=800000, transcendentals=0),
    )(terms, slots)
    count = lax.axis_size("gy")
    hops = [(i, (i + 2) % count if i % 2 == 0 else (i - 2) % count) for i in range(count)]
    yb = lax.ppermute(ya, "gy", hops)
    face = f32((40, 128))
    xa, xb = pl.pallas_call(
        x_kernel,
        out_shape=(face, face),
        in_specs=[VMEM] * 3,
        out_specs=(VMEM,) * 2,
        compiler_params=small,
    )(ya, yb, field)
    field = pl.pallas_call(
        y_kernel,
        out_shape=f32((FROWS, 128)),
        in_specs=[VMEM] * 3,
        out_specs=VMEM,
        input_output_aliases={2: 0},
        compiler_params=small,
        cost_estimate=pl.CostEstimate(flops=1000000, bytes_accessed=800000, transcendentals=0),
    )(ya, yb, field)
    xa = swap(xa, 0, False)
    xb = swap(xb, 0, True)
    face = f32((96, 128))
    field, za, zb = pl.pallas_call(
        z_kernel,
        out_shape=(f32((FROWS, 128)), face, face),
        in_specs=[VMEM] * 3,
        out_specs=(VMEM,) * 3,
        input_output_aliases={2: 0},
        compiler_params=pltpu.CompilerParams(vmem_limit_bytes=8 << 20),
    )(xa, xb, field)
    za = swap(za, 2, False)
    zb = swap(zb, 2, True)
    veloc_out, accel_out = pl.pallas_call(
        end_kernel,
        out_shape=(f32(flat), f32(flat)),
        in_specs=[VMEM] * 4,
        out_specs=(HBM, HBM),
        scratch_shapes=[
            pltpu.VMEM(flat, F32), pltpu.VMEM(flat, F32), pltpu.VMEM((4, 9, 16, 128), F32),
            pltpu.VMEM((4, 16, 640), F32), pltpu.SemaphoreType.DMA((6,)),
        ],
        compiler_params=pltpu.CompilerParams(vmem_limit_bytes=8 << 20),
    )(za, zb, field, v_half)
    shape = (3, 1, 1, 1, NODES)
    return displ_out.reshape(shape), veloc_out.reshape(shape), accel_out.reshape(shape)


def solution(mesh):
    nodal = P(None, "gx", "gy", "gz", None)
    point = P("gx", "gy", "gz", None, None)
    placed = (nodal,) * 3 + (point, P("gx", "gy", "gz", None, None, None)) + (point,) * 4
    return jax.shard_map(
        body, mesh=mesh, in_specs=placed, out_specs=(nodal,) * 3, check_vma=False
    )
```

```python
import functools

import jax
import jax.numpy as jnp
import numpy as np
from jax import lax
from jax.experimental import pallas as pl
from jax.experimental.pallas import tpu as pltpu
from jax.sharding import PartitionSpec as P

EX = 4
EY = 16
EZ = 2
NX = 4 * EX + 1
NY = 4 * EY + 1
NZ = 4 * EZ + 1
NODES = NX * NY * NZ
ROW = NY * NZ
XPAD = 24
FROWS = 960

time_step = 0.1
HALF = 0.5 * time_step
HALF_SQ = 0.5 * time_step * time_step
F32 = jnp.float32
BF16 = jnp.bfloat16
VMEM = pl.BlockSpec(memory_space=pltpu.VMEM)
HBM = pl.BlockSpec(memory_space=pltpu.HBM)


def derivative_table():
    points = np.array([-1.0, -np.sqrt(3.0 / 7.0), 0.0, np.sqrt(3.0 / 7.0), 1.0])
    count = points.shape[0]
    weights = np.array(
        [
            1.0 / np.prod([points[s] - points[o] for o in range(count) if o != s])
            for s in range(count)
        ]
    )
    table = np.zeros((count, count))
    for target in range(count):
        for source in range(count):
            if target != source:
                table[target, source] = (
                    weights[source] / weights[target] / (points[target] - points[source])
                )
        table[target, target] = -np.sum(table[target])
    return table


def operator_tables():
    table = derivative_table().astype(np.float32).astype(np.float64)
    eye = np.eye(5)
    full = np.zeros((3, 128, 128))
    full[0, :125, :125] = np.kron(np.kron(table, eye), eye)
    full[1, :125, :125] = np.kron(np.kron(eye, table), eye)
    full[2, :125, :125] = np.kron(np.kron(eye, eye), table)
    forward = full.reshape(384, 128)
    backward = -np.transpose(full, (2, 0, 1)).reshape(128, 384)
    out = []
    for matrix in (forward, backward):
        high = matrix.astype(np.float32).astype(jnp.bfloat16)
        low = (matrix - high.astype(np.float64)).astype(np.float32).astype(jnp.bfloat16)
        out.append(np.concatenate([high, low], axis=0))
    return out


def split(value):
    high = value.astype(BF16)
    return high, (value - high.astype(F32)).astype(BF16)


def dot(lhs, rhs):
    return lax.dot_general(lhs, rhs, (((1,), (0,)), ((), ())), preferred_element_type=F32)


def take(value, index):
    return jnp.take_along_axis(value, index, axis=1, mode="promise_in_bounds")


def lanes(shape=(8, 128)):
    return lax.broadcasted_iota(jnp.int32, shape, len(shape) - 1)


def force_kernel(
    d_hbm, v_hbm, a_hbm, n_hbm, m_hbm, j_hbm, l_hbm, s_hbm, r_hbm, fw_hbm, bw_hbm,
    t_ref, o_ref, y_ref, vh_ref, pos_s,
    d_s, v_s, a_s, n_s, m_s, j_s, l_s, s_s, r_s, fw_s, bw_s,
    grid_s, nodal_s, local_s, grad_s, fluxh_s, fluxl_s, sems,
):
    copies = []
    moves = [(d_hbm, d_s), (v_hbm, v_s), (a_hbm, a_s), (n_hbm.at[pl.ds(0, 1)], n_s), (fw_hbm, fw_s)]
    for k in range(9):
        moves.append((m_hbm.at[pl.ds(125 * k, 125), 0], m_s.at[k, pl.ds(0, 125)]))
    for src, dst in ((j_hbm, j_s), (l_hbm, l_s), (s_hbm, s_s), (r_hbm, r_s)):
        moves.append((src.at[pl.ds(0, 125), 0], dst.at[pl.ds(0, 125)]))
    moves.append((bw_hbm, bw_s))
    for at, (src, dst) in enumerate(moves):
        copy = pltpu.make_async_copy(src, dst, sems.at[at])
        copy.start()
        copies.append(copy)
    for at in range(4):
        copies[at].wait()
    accel = a_s[...]
    veloc = v_s[...]
    pos_s[...] = d_s[...] + time_step * veloc + HALF_SQ * accel
    vh_ref[...] = veloc + HALF * accel
    lane = lanes()

    corner = jnp.broadcast_to(n_s[0], (8, 128))
    elem_x = (
        (corner >= 2340).astype(jnp.int32)
        + (corner >= 4680).astype(jnp.int32)
        + (corner >= 7020).astype(jnp.int32)
    )
    rest = corner - 2340 * elem_x
    elem_y = jnp.floor((rest.astype(F32) + 0.5) * (1.0 / 36.0)).astype(jnp.int32)
    elem_z = (rest - 36 * elem_y) >> 2
    group = elem_x * 2 + elem_z
    brick = (group * 16 + elem_y).astype(F32)
    column = jnp.broadcast_to(brick[0:1], (128, 128)).T
    hit = column == lanes((128, 128)).astype(F32)
    slot_index = lax.broadcasted_iota(jnp.int32, (128, 128), 0).astype(F32)
    slot_of = jnp.sum(jnp.where(hit, slot_index, 0.0), axis=0, keepdims=True)
    slot_of = jnp.broadcast_to(slot_of, (8, 128)).astype(jnp.int32)

    for m in range(3):
        for x in range(NX):
            value = pos_s[m, :, pl.ds(ROW * x, ROW)]
            if x < 16:
                grid_s[m, x : x + 1, :ROW] = value
            else:
                grid_s[3, m : m + 1, :ROW] = value
    places = [9 * (lane & 63) + 4 * (lane >> 6) + c for c in range(5)]
    for u in range(2):
        c = jnp.minimum(4 * u + (lane >> 5), 4)
        places.append(36 * (lane & 15) + 36 + c + 4 * ((lane >> 4) & 1))
    for m in range(4):
        for tile in range(2 if m < 3 else 1):
            rows = slice(8 * tile, 8 * tile + 8)
            parts = [grid_s[m, rows, 128 * v : 128 * v + 128] for v in range(5)]
            for c in range(7):
                low = places[c] & 127
                high = places[c] >> 7
                got = take(parts[0], low)
                for v in range(1, 5):
                    got = jnp.where(high == v, take(parts[v], low), got)
                if m < 3:
                    nodal_s[m, c, rows, :] = got
                else:
                    for k in range(3):
                        nodal_s[k, c, 16:17, :] = got[k : k + 1]

    masks = [elem_x == x for x in range(4)]
    inner = 64 * elem_z + 4 * elem_y
    outer = 16 * elem_z + elem_y
    for m in range(3):
        local_s[m, 120:128, :] = jnp.zeros((8, 128), F32)
        for c in range(5):
            near = [nodal_s[m, c, 4 * x : 4 * x + 8, :] for x in range(4)]
            last = [nodal_s[m, 5 + c // 4, 4 * x : 4 * x + 8, :] for x in range(4)]
            for b in range(5):
                parts, at = (near, inner + b) if b < 4 else (last, outer + 32 * (c % 4))
                got = take(parts[0], at)
                for x in range(1, 4):
                    got = jnp.where(masks[x], take(parts[x], at), got)
                local_s[m, pl.ds(5 * b + c, 5, stride=25), :] = got[:5]

    copies[4].wait()
    local = jnp.concatenate([local_s[m] for m in range(3)], axis=1)
    high, low = split(local)
    both = dot(fw_s[...], high)
    grad_s[...] = both[:384] + both[384:] + dot(fw_s[0:384, :], low)

    for at in range(5, 18):
        copies[at].wait()
    for chunk in range(8):
        at = 16 * chunk
        rows = slice(at, at + 16)
        g = [
            [grad_s[128 * l + at : 128 * l + at + 16, 128 * c : 128 * c + 128] for c in range(3)]
            for l in range(3)
        ]
        mp = [[m_s[3 * l + j, rows, :] for j in range(3)] for l in range(3)]
        gr = [
            [g[0][c] * mp[0][j] + g[1][c] * mp[1][j] + g[2][c] * mp[2][j] for j in range(3)]
            for c in range(3)
        ]
        mu = s_s[rows, :]
        trace = l_s[rows, :] * (gr[0][0] + gr[1][1] + gr[2][2])
        weight = j_s[rows, :]
        stress = [[None] * 3 for _ in range(3)]
        for c in range(3):
            for j in range(c, 3):
                value = mu * (gr[c][j] + gr[j][c])
                stress[c][j] = stress[j][c] = value + trace if c == j else value
        keep = lax.broadcasted_iota(jnp.int32, (16, 128), 0) < 125 - at
        mass = r_s[rows, :] * weight
        t_ref[3, rows, :] = jnp.where(keep, mass, 0.0) if chunk == 7 else mass
        for l in range(3):
            for c in range(3):
                flux = weight * (
                    stress[c][0] * mp[l][0] + stress[c][1] * mp[l][1] + stress[c][2] * mp[l][2]
                )
                if chunk == 7:
                    flux = jnp.where(keep, flux, 0.0)
                high, low = split(flux)
                to = slice(128 * l + at, 128 * l + at + 16)
                cols = slice(128 * c, 128 * c + 128)
                fluxh_s[to, cols] = high
                fluxl_s[to, cols] = low

    copies[18].wait()
    both = dot(bw_s[...], fluxh_s[...])
    terms = both[:128] + both[128:] + dot(bw_s[0:128, :], fluxl_s[...])
    for m in range(3):
        t_ref[m, 0:128, :] = terms[:, 128 * m : 128 * m + 128]
    for m in range(4):
        t_ref[m, 128:200, :] = jnp.zeros((72, 128), F32)
    o_ref[...] = slot_of

    edge = take(slot_of, 16 * (lane & 7) + 15 * ((lane >> 3) & 1))
    second = ((lane >> 3) & 1) == 1
    packs = []
    for q in range(3):
        pack = jnp.zeros((8, 128), F32)
        for k in range(8 * q, min(8 * q + 8, 20)):
            m, c = divmod(k, 5)
            got = jnp.where(
                second,
                take(t_ref[m, pl.ds(20 + c, 8, stride=25), :], edge),
                take(t_ref[m, pl.ds(c, 8, stride=25), :], edge),
            )
            pack = jnp.where((lane >> 4) == k - 8 * q, got, pack)
        packs.append(pack)
    even = 1 - lax.axis_index("gy") % 2
    upper = (lane >= 64).astype(jnp.int32)
    face = upper + even - 2 * upper * even
    plane = lane - 64 * upper
    comp = (
        (plane >= 9).astype(jnp.int32)
        + (plane >= 18).astype(jnp.int32)
        + (plane >= 27).astype(jnp.int32)
    )
    z = plane - 9 * comp
    row = lax.broadcasted_iota(jnp.int32, (8, 128), 0)
    zero = jnp.zeros((8, 128), F32)
    parts = []
    for x in range(4):
        total = zero
        for h in range(2):
            c = z - 4 * h
            good = (c >= 0) & (c <= 4) & (plane < 36)
            k = 5 * comp + c
            at = (16 * (k & 7) + 8 * face + 2 * x + h) & 127
            for q in range(3):
                total = total + jnp.where(good & ((k >> 3) == q), take(packs[q], at), zero)
        parts.append(total)
    stack_rows(parts, row, zero, y_ref, 0)


def stack_rows(parts, row, zero, out_ref, at):
    second = pltpu.roll(parts[1], 4, 0)
    fourth = pltpu.roll(parts[3], 4, 0)
    out_ref[at : at + 8, :] = parts[0] + jnp.where(row >= 4, second, zero)
    out_ref[at + 8 : at + 16, :] = (
        parts[2] + jnp.where(row < 4, second, zero) + jnp.where(row >= 4, fourth, zero)
    )
    out_ref[at + 16 : at + 24, :] = jnp.where(row < 4, fourth, zero)


def field_kernel(t_ref, o_ref, d_ref, f_ref, d_out, sem):
    out_copy = pltpu.make_async_copy(d_ref, d_out, sem)
    out_copy.start()
    slot_of = o_ref[...]
    lane = lanes()
    gathers = []
    for g in range(8):
        base = 16 * g + (lane >> 2)
        gathers.append(
            (take(slot_of, jnp.minimum(base, 127)), take(slot_of, jnp.clip(base - 1, 0, 127)))
        )
    quarter = lane & 3
    inside = lane < 64
    firsts = [(quarter == b) & inside for b in range(4)]
    lasts = (quarter == 0) & (lane >= 4) & (lane < 68)
    row = lax.broadcasted_iota(jnp.int32, (8, 128), 0)
    zero = jnp.zeros((8, 128), F32)
    for m in range(4):
        planes = {}
        for c in range(5):
            parts = [t_ref[m, pl.ds(5 * b + c, 8, stride=25), :] for b in range(5)]
            for g in range(8):
                at, before = gathers[g]
                got = jnp.where(firsts[0], take(parts[0], at), zero)
                for b in range(1, 4):
                    got = jnp.where(firsts[b], take(parts[b], at), got)
                got = got + jnp.where(lasts, take(parts[4], before), zero)
                key = (4 * (g % 2) + c, g // 2)
                planes[key] = planes[key] + got if key in planes else got
        for z in range(NZ):
            stack_rows([planes[(z, x)] for x in range(4)], row, zero, f_ref, (m * 9 + z) * XPAD)
    f_ref[36 * XPAD : FROWS, :] = jnp.zeros((FROWS - 36 * XPAD, 128), F32)
    out_copy.wait()


def y_faces(ya, yb):
    at = lax.axis_index("gy")
    odd = at % 2 == 1
    outer = (at > 0) & (at < lax.axis_size("gy") - 1)
    far = jnp.where(outer, yb, 0.0)
    return jnp.where(odd, ya, far), jnp.where(odd, far, ya)


def x_kernel(ya_ref, yb_ref, f_ref, xa_ref, xb_ref):
    pad = jnp.zeros((128 - XPAD, 128), F32)
    near = jnp.concatenate([ya_ref[...], pad], axis=0).T[0:40]
    far = jnp.concatenate([yb_ref[...], pad], axis=0).T[64:104]
    lo, hi = y_faces(near, far)
    lane = lanes((40, 128))

    def face(x):
        return (
            f_ref[pl.ds(x, 40, stride=XPAD), :]
            + jnp.where(lane == 0, pltpu.roll(lo, (128 - x) % 128, 1) if x else lo, 0.0)
            + jnp.where(lane == 64, pltpu.roll(hi, 64 - x, 1), 0.0)
        )

    first = face(0)
    last = face(16)
    odd = lax.axis_index("gx") % 2 == 1
    xa_ref[...] = jnp.where(odd, first, last)
    xb_ref[...] = jnp.where(odd, last, first)


def y_kernel(ya_ref, yb_ref, f_in, f_ref):
    lane = lanes()
    for tile in range(3):
        rows = slice(8 * tile, 8 * tile + 8)
        lo, hi = y_faces(ya_ref[rows, :], pltpu.roll(yb_ref[rows, :], 64, 1))
        for plane in range(36):
            to = slice(plane * XPAD + 8 * tile, plane * XPAD + 8 * tile + 8)
            low = pltpu.roll(lo, 128 - plane, 1) if plane else lo
            f_ref[to, :] = (
                f_in[to, :]
                + jnp.where(lane == 0, low, 0.0)
                + jnp.where(lane == 64, pltpu.roll(hi, (64 - plane) % 128, 1), 0.0)
            )


def z_kernel(xa_ref, xb_ref, f_in, f_ref, za_ref, zb_ref):
    at = lax.axis_index("gx")
    odd = at % 2 == 1
    outer = (at > 0) & (at < lax.axis_size("gx") - 1)
    near = xa_ref[0:36, :]
    far = jnp.where(outer, xb_ref[0:36, :], 0.0)
    f_ref[0 : 36 * XPAD, :] = f_in[0 : 36 * XPAD, :]
    f_ref[pl.ds(0, 36, stride=XPAD), :] = f_in[pl.ds(0, 36, stride=XPAD), :] + jnp.where(
        odd, near, far
    )
    f_ref[pl.ds(16, 36, stride=XPAD), :] = f_in[pl.ds(16, 36, stride=XPAD), :] + jnp.where(
        odd, far, near
    )
    odd = lax.axis_index("gz") % 2 == 1
    for m in range(4):
        at = m * 9 * XPAD
        first = f_ref[at : at + XPAD, :]
        last = f_ref[at + 8 * XPAD : at + 9 * XPAD, :]
        za_ref[XPAD * m : XPAD * m + XPAD, :] = jnp.where(odd, first, last)
        zb_ref[XPAD * m : XPAD * m + XPAD, :] = jnp.where(odd, last, first)


def row_spots(lane):
    spots = []
    for v in range(5):
        at = lane + 128 * v
        y = jnp.floor((at.astype(F32) + 0.5) * (1.0 / 9.0)).astype(jnp.int32)
        spots.append((y, at - 9 * y))
    return spots


def inner_kernel(f_ref, grid_ref, acc_s):
    for z in range(1, 8):
        for tile in range(3):
            rows = [(m * 9 + z) * XPAD + 8 * tile for m in range(4)]
            mass = f_ref[rows[3] : rows[3] + 8, :]
            for m in range(3):
                value = f_ref[rows[m] : rows[m] + 8, :] / mass
                if tile < 2:
                    acc_s[m, z, 8 * tile : 8 * tile + 8, :] = value
                else:
                    acc_s[3, z, m : m + 1, :] = value[0:1]
    spots = row_spots(lanes())
    for m in range(4):
        for tile in range(2 if m < 3 else 1):
            rows = slice(8 * tile, 8 * tile + 8)
            for v in range(5):
                y, z_of = spots[v]
                got = take(acc_s[m, 1, rows, :], y)
                for z in range(2, 8):
                    got = jnp.where(z_of == z, take(acc_s[m, z, rows, :], y), got)
                grid_ref[m, rows, 128 * v : 128 * v + 128] = got
    grid_ref[3, 8:16, :] = jnp.zeros((8, 640), F32)


def end_kernel(
    za_ref, zb_ref, f_ref, vh_ref, inner_ref, v_out, a_out, a_s, v_s, acc_s, grid_s, sems
):
    at = lax.axis_index("gz")
    odd = at % 2 == 1
    outer = (at > 0) & (at < lax.axis_size("gz") - 1)
    spots = row_spots(lanes())

    def added(m, z, tile):
        at = (m * 9 + z) * XPAD + 8 * tile
        rows = slice(XPAD * m + 8 * tile, XPAD * m + 8 * tile + 8)
        near = za_ref[rows, :]
        far = jnp.where(outer, zb_ref[rows, :], 0.0)
        return f_ref[at : at + 8, :] + (
            jnp.where(odd, near, far) if z == 0 else jnp.where(odd, far, near)
        )

    def to_rows(m, tile):
        rows = slice(8 * tile, 8 * tile + 8)
        for v in range(5):
            y, z_of = spots[v]
            cols = slice(128 * v, 128 * v + 128)
            got = jnp.where(z_of == 0, take(acc_s[m, 0, rows, :], y), inner_ref[m, rows, cols])
            got = jnp.where(z_of == 8, take(acc_s[m, 1, rows, :], y), got)
            grid_s[m, rows, cols] = got

    for z in (0, 8):
        for tile in range(3):
            mass = added(3, z, tile)
            for m in range(3):
                value = added(m, z, tile) / mass
                if tile < 2:
                    acc_s[m, z // 8, 8 * tile : 8 * tile + 8, :] = value
                else:
                    acc_s[3, z // 8, m : m + 1, :] = value[0:1]
    to_rows(3, 0)
    for m in range(3):
        to_rows(m, 0)
        to_rows(m, 1)
        for x in range(16):
            a_s[m, :, pl.ds(ROW * x, ROW)] = grid_s[m, x : x + 1, :ROW]
        a_s[m, :, pl.ds(ROW * 16, ROW)] = grid_s[3, m : m + 1, :ROW]
    a_copy = pltpu.make_async_copy(a_s, a_out, sems.at[0])
    a_copy.start()
    v_s[...] = vh_ref[...] + HALF * a_s[...]
    v_copy = pltpu.make_async_copy(v_s, v_out, sems.at[1])
    v_copy.start()
    a_copy.wait()
    v_copy.wait()


def swap(value, at, second):
    axes = ("gx", "gy", "gz")
    sizes = [lax.axis_size(axis) for axis in axes]
    other = 0 if at == 2 else 2
    pairs = []
    for index in np.ndindex(*sizes):
        target = list(index)
        if not second:
            target[at] ^= 1
        elif 0 < index[at] < sizes[at] - 1:
            target[at] = ((index[at] - 1) ^ 1) + 1
        else:
            target[other] ^= 1
        pairs.append(tuple(int(np.ravel_multi_index(i, sizes)) for i in (index, target)))
    return lax.ppermute(value, axes, pairs)


def body(displ, veloc, accel, node_index, inv_map, jac_weight, lame_first, shear_mod, density):
    f32 = functools.partial(jax.ShapeDtypeStruct, dtype=F32)
    flat = (3, 1, NODES)
    points = (125, 1, 128)
    tables = [jnp.asarray(table) for table in operator_tables()]
    scratch = [
        pltpu.VMEM(flat, F32), pltpu.VMEM(flat, F32), pltpu.VMEM(flat, F32),
        pltpu.VMEM((1, 1, 128), jnp.int32),
        pltpu.VMEM((9, 128, 128), F32),
        pltpu.VMEM((128, 128), F32), pltpu.VMEM((128, 128), F32),
        pltpu.VMEM((128, 128), F32), pltpu.VMEM((128, 128), F32),
        pltpu.VMEM((768, 128), BF16), pltpu.VMEM((256, 384), BF16),
        pltpu.VMEM((4, 16, 640), F32), pltpu.VMEM((3, 7, 24, 128), F32),
        pltpu.VMEM((3, 128, 128), F32), pltpu.VMEM((384, 384), F32),
        pltpu.VMEM((384, 384), BF16), pltpu.VMEM((384, 384), BF16),
        pltpu.SemaphoreType.DMA((19,)),
    ]
    terms, slots, ya, v_half, displ_new = pl.pallas_call(
        force_kernel,
        out_shape=(
            f32((4, 200, 128)), jax.ShapeDtypeStruct((8, 128), jnp.int32), f32((XPAD, 128)),
            f32(flat), f32(flat),
        ),
        in_specs=[HBM] * 11,
        out_specs=(VMEM,) * 5,
        scratch_shapes=scratch,
        compiler_params=pltpu.CompilerParams(vmem_limit_bytes=16 << 20),
    )(
        *(
            pltpu.with_memory_space_constraint(value, pltpu.HBM)
            for value in (
                displ.reshape(flat), veloc.reshape(flat), accel.reshape(flat),
                node_index.reshape(points), inv_map.reshape(1125, 1, 128),
                jac_weight.reshape(points), lame_first.reshape(points), shear_mod.reshape(points),
                density.reshape(points), *tables,
            )
        )
    )
    small = pltpu.CompilerParams(vmem_limit_bytes=8 << 20)
    ya = swap(ya, 1, False)
    field, displ_out = pl.pallas_call(
        field_kernel,
        out_shape=(f32((FROWS, 128)), f32(flat)),
        in_specs=[VMEM] * 3,
        out_specs=(VMEM, HBM),
        scratch_shapes=[pltpu.SemaphoreType.DMA],
        compiler_params=small,
        cost_estimate=pl.CostEstimate(flops=4000000, bytes_accessed=800000, transcendentals=0),
    )(terms, slots, displ_new)
    count = lax.axis_size("gy")
    hops = [(i, (i + 2) % count if i % 2 == 0 else (i - 2) % count) for i in range(count)]
    yb = lax.ppermute(ya, "gy", hops)
    face = f32((40, 128))
    xa, xb = pl.pallas_call(
        x_kernel,
        out_shape=(face, face),
        in_specs=[VMEM] * 3,
        out_specs=(VMEM,) * 2,
        compiler_params=small,
    )(ya, yb, field)
    field = pl.pallas_call(
        y_kernel,
        out_shape=f32((FROWS, 128)),
        in_specs=[VMEM] * 3,
        out_specs=VMEM,
        input_output_aliases={2: 0},
        compiler_params=small,
        cost_estimate=pl.CostEstimate(flops=1000000, bytes_accessed=800000, transcendentals=0),
    )(ya, yb, field)
    xa = swap(xa, 0, False)
    xb = swap(xb, 0, True)
    face = f32((96, 128))
    field, za, zb = pl.pallas_call(
        z_kernel,
        out_shape=(f32((FROWS, 128)), face, face),
        in_specs=[VMEM] * 3,
        out_specs=(VMEM,) * 3,
        input_output_aliases={2: 0},
        compiler_params=pltpu.CompilerParams(vmem_limit_bytes=8 << 20),
    )(xa, xb, field)
    za = swap(za, 2, False)
    zb = swap(zb, 2, True)
    inner = pl.pallas_call(
        inner_kernel,
        out_shape=f32((4, 16, 640)),
        in_specs=[VMEM],
        out_specs=VMEM,
        scratch_shapes=[pltpu.VMEM((4, 9, 16, 128), F32)],
        compiler_params=small,
        cost_estimate=pl.CostEstimate(flops=1000000, bytes_accessed=800000, transcendentals=0),
    )(field)
    veloc_out, accel_out = pl.pallas_call(
        end_kernel,
        out_shape=(f32(flat), f32(flat)),
        in_specs=[VMEM] * 5,
        out_specs=(HBM, HBM),
        scratch_shapes=[
            pltpu.VMEM(flat, F32), pltpu.VMEM(flat, F32), pltpu.VMEM((4, 2, 16, 128), F32),
            pltpu.VMEM((4, 16, 640), F32), pltpu.SemaphoreType.DMA((2,)),
        ],
        compiler_params=pltpu.CompilerParams(vmem_limit_bytes=8 << 20),
    )(za, zb, field, v_half, inner)
    shape = (3, 1, 1, 1, NODES)
    return displ_out.reshape(shape), veloc_out.reshape(shape), accel_out.reshape(shape)


def solution(mesh):
    nodal = P(None, "gx", "gy", "gz", None)
    point = P("gx", "gy", "gz", None, None)
    placed = (nodal,) * 3 + (point, P("gx", "gy", "gz", None, None, None)) + (point,) * 4
    return jax.shard_map(
        body, mesh=mesh, in_specs=placed, out_specs=(nodal,) * 3, check_vma=False
    )
```

```python
import functools

import jax
import jax.numpy as jnp
import numpy as np
from jax import lax
from jax.experimental import pallas as pl
from jax.experimental.pallas import tpu as pltpu
from jax.sharding import PartitionSpec as P

EX = 4
EY = 16
EZ = 2
NX = 4 * EX + 1
NY = 4 * EY + 1
NZ = 4 * EZ + 1
NODES = NX * NY * NZ
ROW = NY * NZ
XPAD = 24
FROWS = 960

time_step = 0.1
HALF = 0.5 * time_step
HALF_SQ = 0.5 * time_step * time_step
F32 = jnp.float32
BF16 = jnp.bfloat16
VMEM = pl.BlockSpec(memory_space=pltpu.VMEM)
HBM = pl.BlockSpec(memory_space=pltpu.HBM)


def derivative_table():
    points = np.array([-1.0, -np.sqrt(3.0 / 7.0), 0.0, np.sqrt(3.0 / 7.0), 1.0])
    count = points.shape[0]
    weights = np.array(
        [
            1.0 / np.prod([points[s] - points[o] for o in range(count) if o != s])
            for s in range(count)
        ]
    )
    table = np.zeros((count, count))
    for target in range(count):
        for source in range(count):
            if target != source:
                table[target, source] = (
                    weights[source] / weights[target] / (points[target] - points[source])
                )
        table[target, target] = -np.sum(table[target])
    return table


def operator_tables():
    table = derivative_table().astype(np.float32).astype(np.float64)
    eye = np.eye(5)
    full = np.zeros((3, 128, 128))
    full[0, :125, :125] = np.kron(np.kron(table, eye), eye)
    full[1, :125, :125] = np.kron(np.kron(eye, table), eye)
    full[2, :125, :125] = np.kron(np.kron(eye, eye), table)
    forward = full.reshape(384, 128)
    backward = -np.transpose(full, (2, 0, 1)).reshape(128, 384)
    out = []
    for matrix in (forward, backward):
        high = matrix.astype(np.float32).astype(jnp.bfloat16)
        low = (matrix - high.astype(np.float64)).astype(np.float32).astype(jnp.bfloat16)
        out.append((high, low))
    (forward_h, forward_l), (backward_h, backward_l) = out
    return (
        np.concatenate([forward_h, forward_l, forward_h], axis=1),
        np.concatenate([backward_h, backward_l], axis=0),
    )


def split(value):
    high = value.astype(BF16)
    return high, (value - high.astype(F32)).astype(BF16)


def dot(lhs, rhs):
    return lax.dot_general(lhs, rhs, (((1,), (0,)), ((), ())), preferred_element_type=F32)


def take(value, index):
    return jnp.take_along_axis(value, index, axis=1, mode="promise_in_bounds")


def lanes(shape=(8, 128)):
    return lax.broadcasted_iota(jnp.int32, shape, len(shape) - 1)


def force_kernel(
    d_hbm, v_hbm, a_hbm, n_hbm, m_hbm, j_hbm, l_hbm, s_hbm, r_hbm, fw_hbm, bw_hbm,
    t_ref, o_ref, y_ref, vh_ref, pos_s,
    d_s, v_s, a_s, n_s, m_s, j_s, l_s, s_s, r_s, fw_s, bw_s,
    grid_s, nodal_s, local_s, grad_s, fluxh_s, fluxl_s, sems,
):
    copies = []
    moves = [(n_hbm.at[pl.ds(0, 1)], n_s)]
    for src, dst in ((d_hbm, d_s), (v_hbm, v_s), (a_hbm, a_s)):
        moves += [(src.at[m], dst.at[m]) for m in range(3)]
    moves.append((fw_hbm, fw_s))
    for k in range(9):
        moves.append((m_hbm.at[pl.ds(125 * k, 125), 0], m_s.at[k, pl.ds(0, 125)]))
    for src, dst in ((j_hbm, j_s), (l_hbm, l_s), (s_hbm, s_s), (r_hbm, r_s)):
        moves.append((src.at[pl.ds(0, 125), 0], dst.at[pl.ds(0, 125)]))
    moves.append((bw_hbm, bw_s))
    for at, (src, dst) in enumerate(moves):
        copy = pltpu.make_async_copy(src, dst, sems.at[at])
        copy.start()
        copies.append(copy)
    for at in range(10):
        copies[at].wait()
    accel = a_s[...]
    veloc = v_s[...]
    pos_s[...] = d_s[...] + time_step * veloc + HALF_SQ * accel
    vh_ref[...] = veloc + HALF * accel
    lane = lanes()

    corner = jnp.broadcast_to(n_s[0], (8, 128))
    elem_x = (
        (corner >= 2340).astype(jnp.int32)
        + (corner >= 4680).astype(jnp.int32)
        + (corner >= 7020).astype(jnp.int32)
    )
    rest = corner - 2340 * elem_x
    elem_y = jnp.floor((rest.astype(F32) + 0.5) * (1.0 / 36.0)).astype(jnp.int32)
    elem_z = (rest - 36 * elem_y) >> 2
    group = elem_x * 2 + elem_z
    brick = (group * 16 + elem_y).astype(F32)
    column = jnp.broadcast_to(brick[0:1], (128, 128)).T
    hit = column == lanes((128, 128)).astype(F32)
    slot_index = lax.broadcasted_iota(jnp.int32, (128, 128), 0).astype(F32)
    slot_of = jnp.sum(jnp.where(hit, slot_index, 0.0), axis=0, keepdims=True)
    slot_of = jnp.broadcast_to(slot_of, (8, 128)).astype(jnp.int32)

    for m in range(3):
        for x in range(NX):
            value = pos_s[m, :, pl.ds(ROW * x, ROW)]
            if x < 16:
                grid_s[m, x : x + 1, :ROW] = value
            else:
                grid_s[3, m : m + 1, :ROW] = value
    places = [9 * (lane & 63) + 4 * (lane >> 6) + c for c in range(5)]
    for u in range(2):
        c = jnp.minimum(4 * u + (lane >> 5), 4)
        places.append(36 * (lane & 15) + 36 + c + 4 * ((lane >> 4) & 1))
    for m in range(4):
        for tile in range(2 if m < 3 else 1):
            rows = slice(8 * tile, 8 * tile + 8)
            parts = [grid_s[m, rows, 128 * v : 128 * v + 128] for v in range(5)]
            for c in range(7):
                low = places[c] & 127
                high = places[c] >> 7
                got = take(parts[0], low)
                for v in range(1, 5):
                    got = jnp.where(high == v, take(parts[v], low), got)
                if m < 3:
                    nodal_s[m, c, rows, :] = got
                else:
                    for k in range(3):
                        nodal_s[k, c, 16:17, :] = got[k : k + 1]

    masks = [elem_x == x for x in range(4)]
    inner = 64 * elem_z + 4 * elem_y
    outer = 16 * elem_z + elem_y
    for m in range(3):
        local_s[m, 120:128, :] = jnp.zeros((8, 128), F32)
        for c in range(5):
            near = [nodal_s[m, c, 4 * x : 4 * x + 8, :] for x in range(4)]
            last = [nodal_s[m, 5 + c // 4, 4 * x : 4 * x + 8, :] for x in range(4)]
            for b in range(5):
                parts, at = (near, inner + b) if b < 4 else (last, outer + 32 * (c % 4))
                got = take(parts[0], at)
                for x in range(1, 4):
                    got = jnp.where(masks[x], take(parts[x], at), got)
                local_s[m, pl.ds(5 * b + c, 5, stride=25), :] = got[:5]

    copies[10].wait()
    local = jnp.concatenate([local_s[m] for m in range(3)], axis=1)
    high, low = split(local)
    grad_s[...] = dot(fw_s[...], jnp.concatenate([high, high, low], axis=0))

    for at in range(11, 24):
        copies[at].wait()
    for chunk in range(8):
        at = 16 * chunk
        rows = slice(at, at + 16)
        g = [
            [grad_s[128 * l + at : 128 * l + at + 16, 128 * c : 128 * c + 128] for c in range(3)]
            for l in range(3)
        ]
        mp = [[m_s[3 * l + j, rows, :] for j in range(3)] for l in range(3)]
        gr = [
            [g[0][c] * mp[0][j] + g[1][c] * mp[1][j] + g[2][c] * mp[2][j] for j in range(3)]
            for c in range(3)
        ]
        mu = s_s[rows, :]
        trace = l_s[rows, :] * (gr[0][0] + gr[1][1] + gr[2][2])
        weight = j_s[rows, :]
        stress = [[None] * 3 for _ in range(3)]
        for c in range(3):
            for j in range(c, 3):
                value = mu * (gr[c][j] + gr[j][c])
                stress[c][j] = stress[j][c] = value + trace if c == j else value
        keep = lax.broadcasted_iota(jnp.int32, (16, 128), 0) < 125 - at
        mass = r_s[rows, :] * weight
        t_ref[3, rows, :] = jnp.where(keep, mass, 0.0) if chunk == 7 else mass
        for l in range(3):
            for c in range(3):
                flux = weight * (
                    stress[c][0] * mp[l][0] + stress[c][1] * mp[l][1] + stress[c][2] * mp[l][2]
                )
                if chunk == 7:
                    flux = jnp.where(keep, flux, 0.0)
                high, low = split(flux)
                to = slice(128 * l + at, 128 * l + at + 16)
                cols = slice(128 * c, 128 * c + 128)
                fluxh_s[to, cols] = high
                fluxl_s[to, cols] = low

    copies[24].wait()
    both = dot(bw_s[...], fluxh_s[...])
    terms = both[:128] + both[128:] + dot(bw_s[0:128, :], fluxl_s[...])
    for m in range(3):
        t_ref[m, 0:128, :] = terms[:, 128 * m : 128 * m + 128]
    for m in range(4):
        t_ref[m, 128:200, :] = jnp.zeros((72, 128), F32)
    o_ref[...] = slot_of

    edge = take(slot_of, 16 * (lane & 7) + 15 * ((lane >> 3) & 1))
    second = ((lane >> 3) & 1) == 1
    packs = []
    for q in range(3):
        pack = jnp.zeros((8, 128), F32)
        for k in range(8 * q, min(8 * q + 8, 20)):
            m, c = divmod(k, 5)
            got = jnp.where(
                second,
                take(t_ref[m, pl.ds(20 + c, 8, stride=25), :], edge),
                take(t_ref[m, pl.ds(c, 8, stride=25), :], edge),
            )
            pack = jnp.where((lane >> 4) == k - 8 * q, got, pack)
        packs.append(pack)
    even = 1 - lax.axis_index("gy") % 2
    upper = (lane >= 64).astype(jnp.int32)
    face = upper + even - 2 * upper * even
    plane = lane - 64 * upper
    comp = (
        (plane >= 9).astype(jnp.int32)
        + (plane >= 18).astype(jnp.int32)
        + (plane >= 27).astype(jnp.int32)
    )
    z = plane - 9 * comp
    row = lax.broadcasted_iota(jnp.int32, (8, 128), 0)
    zero = jnp.zeros((8, 128), F32)
    parts = []
    for x in range(4):
        total = zero
        for h in range(2):
            c = z - 4 * h
            good = (c >= 0) & (c <= 4) & (plane < 36)
            k = 5 * comp + c
            at = (16 * (k & 7) + 8 * face + 2 * x + h) & 127
            for q in range(3):
                total = total + jnp.where(good & ((k >> 3) == q), take(packs[q], at), zero)
        parts.append(total)
    stack_rows(parts, row, zero, y_ref, 0)


def stack_rows(parts, row, zero, out_ref, at):
    second = pltpu.roll(parts[1], 4, 0)
    fourth = pltpu.roll(parts[3], 4, 0)
    out_ref[at : at + 8, :] = parts[0] + jnp.where(row >= 4, second, zero)
    out_ref[at + 8 : at + 16, :] = (
        parts[2] + jnp.where(row < 4, second, zero) + jnp.where(row >= 4, fourth, zero)
    )
    out_ref[at + 16 : at + 24, :] = jnp.where(row < 4, fourth, zero)


def field_kernel(t_ref, o_ref, f_ref):
    slot_of = o_ref[...]
    lane = lanes()
    gathers = []
    for g in range(8):
        base = 16 * g + (lane >> 2)
        gathers.append(
            (take(slot_of, jnp.minimum(base, 127)), take(slot_of, jnp.clip(base - 1, 0, 127)))
        )
    quarter = lane & 3
    inside = lane < 64
    firsts = [(quarter == b) & inside for b in range(4)]
    lasts = (quarter == 0) & (lane >= 4) & (lane < 68)
    row = lax.broadcasted_iota(jnp.int32, (8, 128), 0)
    zero = jnp.zeros((8, 128), F32)
    for m in range(4):
        planes = {}
        for c in range(5):
            parts = [t_ref[m, pl.ds(5 * b + c, 8, stride=25), :] for b in range(5)]
            for g in range(8):
                at, before = gathers[g]
                got = jnp.where(firsts[0], take(parts[0], at), zero)
                for b in range(1, 4):
                    got = jnp.where(firsts[b], take(parts[b], at), got)
                got = got + jnp.where(lasts, take(parts[4], before), zero)
                key = (4 * (g % 2) + c, g // 2)
                planes[key] = planes[key] + got if key in planes else got
        for z in range(NZ):
            stack_rows([planes[(z, x)] for x in range(4)], row, zero, f_ref, (m * 9 + z) * XPAD)
    f_ref[36 * XPAD : FROWS, :] = jnp.zeros((FROWS - 36 * XPAD, 128), F32)


def y_faces(near, far):
    at = lax.axis_index("gy")
    odd = at % 2 == 1
    outer = (at > 0) & (at < lax.axis_size("gy") - 1)
    far = jnp.where(outer, far, 0.0)
    return jnp.where(odd, near, far), jnp.where(odd, far, near)


def x_kernel(y_ref, f_ref, xa_ref, xb_ref):
    pad = jnp.zeros((128 - XPAD, 128), F32)
    both = jnp.concatenate([y_ref[...], pad], axis=0).T
    lo, hi = y_faces(both[0:40], both[64:104])
    lane = lanes((40, 128))

    def face(x):
        return (
            f_ref[pl.ds(x, 40, stride=XPAD), :]
            + jnp.where(lane == 0, pltpu.roll(lo, (128 - x) % 128, 1) if x else lo, 0.0)
            + jnp.where(lane == 64, pltpu.roll(hi, 64 - x, 1), 0.0)
        )

    first = face(0)
    last = face(16)
    odd = lax.axis_index("gx") % 2 == 1
    xa_ref[...] = jnp.where(odd, first, last)
    xb_ref[...] = jnp.where(odd, last, first)


def y_kernel(y_ref, f_in, f_ref):
    lane = lanes()
    for tile in range(3):
        rows = slice(8 * tile, 8 * tile + 8)
        lo, hi = y_faces(y_ref[rows, :], pltpu.roll(y_ref[rows, :], 64, 1))
        for plane in range(36):
            to = slice(plane * XPAD + 8 * tile, plane * XPAD + 8 * tile + 8)
            low = pltpu.roll(lo, 128 - plane, 1) if plane else lo
            f_ref[to, :] = (
                f_in[to, :]
                + jnp.where(lane == 0, low, 0.0)
                + jnp.where(lane == 64, pltpu.roll(hi, (64 - plane) % 128, 1), 0.0)
            )


def z_kernel(xa_ref, xb_ref, f_in, f_ref, za_ref, zb_ref):
    at = lax.axis_index("gx")
    odd = at % 2 == 1
    outer = (at > 0) & (at < lax.axis_size("gx") - 1)
    near = xa_ref[0:36, :]
    far = jnp.where(outer, xb_ref[0:36, :], 0.0)
    f_ref[0 : 36 * XPAD, :] = f_in[0 : 36 * XPAD, :]
    f_ref[pl.ds(0, 36, stride=XPAD), :] = f_in[pl.ds(0, 36, stride=XPAD), :] + jnp.where(
        odd, near, far
    )
    f_ref[pl.ds(16, 36, stride=XPAD), :] = f_in[pl.ds(16, 36, stride=XPAD), :] + jnp.where(
        odd, far, near
    )
    odd = lax.axis_index("gz") % 2 == 1
    for m in range(4):
        at = m * 9 * XPAD
        first = f_ref[at : at + XPAD, :]
        last = f_ref[at + 8 * XPAD : at + 9 * XPAD, :]
        za_ref[XPAD * m : XPAD * m + XPAD, :] = jnp.where(odd, first, last)
        zb_ref[XPAD * m : XPAD * m + XPAD, :] = jnp.where(odd, last, first)


def row_spots(lane):
    spots = []
    for v in range(5):
        at = lane + 128 * v
        y = jnp.floor((at.astype(F32) + 0.5) * (1.0 / 9.0)).astype(jnp.int32)
        spots.append((y, at - 9 * y))
    return spots


def inner_kernel(f_ref, d_ref, grid_ref, d_out, acc_s, sem):
    out_copy = pltpu.make_async_copy(d_ref, d_out, sem)
    out_copy.start()
    for z in range(1, 8):
        for tile in range(3):
            rows = [(m * 9 + z) * XPAD + 8 * tile for m in range(4)]
            mass = f_ref[rows[3] : rows[3] + 8, :]
            for m in range(3):
                value = f_ref[rows[m] : rows[m] + 8, :] / mass
                if tile < 2:
                    acc_s[m, z, 8 * tile : 8 * tile + 8, :] = value
                else:
                    acc_s[3, z, m : m + 1, :] = value[0:1]
    spots = row_spots(lanes())
    for m in range(4):
        for tile in range(2 if m < 3 else 1):
            rows = slice(8 * tile, 8 * tile + 8)
            for v in range(5):
                y, z_of = spots[v]
                got = take(acc_s[m, 1, rows, :], y)
                for z in range(2, 8):
                    got = jnp.where(z_of == z, take(acc_s[m, z, rows, :], y), got)
                grid_ref[m, rows, 128 * v : 128 * v + 128] = got
    grid_ref[3, 8:16, :] = jnp.zeros((8, 640), F32)
    out_copy.wait()


def end_kernel(
    za_ref, zb_ref, f_ref, vh_ref, inner_ref, v_out, a_out, a_s, v_s, acc_s, grid_s, sems
):
    at = lax.axis_index("gz")
    odd = at % 2 == 1
    outer = (at > 0) & (at < lax.axis_size("gz") - 1)
    spots = row_spots(lanes())

    def added(m, z, tile):
        at = (m * 9 + z) * XPAD + 8 * tile
        rows = slice(XPAD * m + 8 * tile, XPAD * m + 8 * tile + 8)
        near = za_ref[rows, :]
        far = jnp.where(outer, zb_ref[rows, :], 0.0)
        return f_ref[at : at + 8, :] + (
            jnp.where(odd, near, far) if z == 0 else jnp.where(odd, far, near)
        )

    def to_rows(m, tile):
        rows = slice(8 * tile, 8 * tile + 8)
        for v in range(5):
            y, z_of = spots[v]
            cols = slice(128 * v, 128 * v + 128)
            got = jnp.where(z_of == 0, take(acc_s[m, 0, rows, :], y), inner_ref[m, rows, cols])
            got = jnp.where(z_of == 8, take(acc_s[m, 1, rows, :], y), got)
            grid_s[m, rows, cols] = got

    for z in (0, 8):
        for tile in range(3):
            mass = added(3, z, tile)
            for m in range(3):
                value = added(m, z, tile) / mass
                if tile < 2:
                    acc_s[m, z // 8, 8 * tile : 8 * tile + 8, :] = value
                else:
                    acc_s[3, z // 8, m : m + 1, :] = value[0:1]
    to_rows(3, 0)
    for m in range(3):
        to_rows(m, 0)
        to_rows(m, 1)
        for x in range(16):
            a_s[m, :, pl.ds(ROW * x, ROW)] = grid_s[m, x : x + 1, :ROW]
        a_s[m, :, pl.ds(ROW * 16, ROW)] = grid_s[3, m : m + 1, :ROW]
    a_copy = pltpu.make_async_copy(a_s, a_out, sems.at[0])
    a_copy.start()
    v_s[...] = vh_ref[...] + HALF * a_s[...]
    v_copy = pltpu.make_async_copy(v_s, v_out, sems.at[1])
    v_copy.start()
    a_copy.wait()
    v_copy.wait()


def swap(value, at, second):
    axes = ("gx", "gy", "gz")
    sizes = [lax.axis_size(axis) for axis in axes]
    other = 0 if at == 2 else 2
    pairs = []
    for index in np.ndindex(*sizes):
        target = list(index)
        if not second:
            target[at] ^= 1
        elif 0 < index[at] < sizes[at] - 1:
            target[at] = ((index[at] - 1) ^ 1) + 1
        else:
            target[other] ^= 1
        pairs.append(tuple(int(np.ravel_multi_index(i, sizes)) for i in (index, target)))
    return lax.ppermute(value, axes, pairs)


def body(displ, veloc, accel, node_index, inv_map, jac_weight, lame_first, shear_mod, density):
    f32 = functools.partial(jax.ShapeDtypeStruct, dtype=F32)
    flat = (3, 1, NODES)
    points = (125, 1, 128)
    tables = [jnp.asarray(table) for table in operator_tables()]
    scratch = [
        pltpu.VMEM(flat, F32), pltpu.VMEM(flat, F32), pltpu.VMEM(flat, F32),
        pltpu.VMEM((1, 1, 128), jnp.int32),
        pltpu.VMEM((9, 128, 128), F32),
        pltpu.VMEM((128, 128), F32), pltpu.VMEM((128, 128), F32),
        pltpu.VMEM((128, 128), F32), pltpu.VMEM((128, 128), F32),
        pltpu.VMEM((384, 384), BF16), pltpu.VMEM((256, 384), BF16),
        pltpu.VMEM((4, 16, 640), F32), pltpu.VMEM((3, 7, 24, 128), F32),
        pltpu.VMEM((3, 128, 128), F32), pltpu.VMEM((384, 384), F32),
        pltpu.VMEM((384, 384), BF16), pltpu.VMEM((384, 384), BF16),
        pltpu.SemaphoreType.DMA((25,)),
    ]
    terms, slots, ya, v_half, displ_new = pl.pallas_call(
        force_kernel,
        out_shape=(
            f32((4, 200, 128)), jax.ShapeDtypeStruct((8, 128), jnp.int32), f32((XPAD, 128)),
            f32(flat), f32(flat),
        ),
        in_specs=[HBM] * 11,
        out_specs=(VMEM,) * 5,
        scratch_shapes=scratch,
        compiler_params=pltpu.CompilerParams(vmem_limit_bytes=16 << 20),
    )(
        *(
            pltpu.with_memory_space_constraint(value, pltpu.HBM)
            for value in (
                displ.reshape(flat), veloc.reshape(flat), accel.reshape(flat),
                node_index.reshape(points), inv_map.reshape(1125, 1, 128),
                jac_weight.reshape(points), lame_first.reshape(points), shear_mod.reshape(points),
                density.reshape(points), *tables,
            )
        )
    )
    small = pltpu.CompilerParams(vmem_limit_bytes=8 << 20)
    count = lax.axis_size("gy")
    hops = [(i, (i - 2) % count if i % 2 == 0 else (i + 2) % count) for i in range(count)]
    passed = lax.ppermute(ya, "gy", hops)
    ya = swap(jnp.where(lanes((XPAD, 128)) < 64, ya, passed), 1, False)
    field = pl.pallas_call(
        field_kernel,
        out_shape=f32((FROWS, 128)),
        in_specs=[VMEM] * 2,
        out_specs=VMEM,
        compiler_params=small,
        cost_estimate=pl.CostEstimate(flops=4000000, bytes_accessed=800000, transcendentals=0),
    )(terms, slots)
    face = f32((40, 128))
    xa, xb = pl.pallas_call(
        x_kernel,
        out_shape=(face, face),
        in_specs=[VMEM] * 2,
        out_specs=(VMEM,) * 2,
        compiler_params=small,
    )(ya, field)
    field = pl.pallas_call(
        y_kernel,
        out_shape=f32((FROWS, 128)),
        in_specs=[VMEM] * 2,
        out_specs=VMEM,
        input_output_aliases={1: 0},
        compiler_params=small,
        cost_estimate=pl.CostEstimate(flops=1000000, bytes_accessed=800000, transcendentals=0),
    )(ya, field)
    xa = swap(xa, 0, False)
    xb = swap(xb, 0, True)
    face = f32((96, 128))
    field, za, zb = pl.pallas_call(
        z_kernel,
        out_shape=(f32((FROWS, 128)), face, face),
        in_specs=[VMEM] * 3,
        out_specs=(VMEM,) * 3,
        input_output_aliases={2: 0},
        compiler_params=pltpu.CompilerParams(vmem_limit_bytes=8 << 20),
    )(xa, xb, field)
    za = swap(za, 2, False)
    zb = swap(zb, 2, True)
    inner, displ_out = pl.pallas_call(
        inner_kernel,
        out_shape=(f32((4, 16, 640)), f32(flat)),
        in_specs=[VMEM] * 2,
        out_specs=(VMEM, HBM),
        scratch_shapes=[pltpu.VMEM((4, 9, 16, 128), F32), pltpu.SemaphoreType.DMA],
        compiler_params=small,
        cost_estimate=pl.CostEstimate(flops=1000000, bytes_accessed=800000, transcendentals=0),
    )(field, displ_new)
    veloc_out, accel_out = pl.pallas_call(
        end_kernel,
        out_shape=(f32(flat), f32(flat)),
        in_specs=[VMEM] * 5,
        out_specs=(HBM, HBM),
        scratch_shapes=[
            pltpu.VMEM(flat, F32), pltpu.VMEM(flat, F32), pltpu.VMEM((4, 2, 16, 128), F32),
            pltpu.VMEM((4, 16, 640), F32), pltpu.SemaphoreType.DMA((2,)),
        ],
        compiler_params=pltpu.CompilerParams(vmem_limit_bytes=8 << 20),
    )(za, zb, field, v_half, inner)
    shape = (3, 1, 1, 1, NODES)
    return displ_out.reshape(shape), veloc_out.reshape(shape), accel_out.reshape(shape)


def solution(mesh):
    nodal = P(None, "gx", "gy", "gz", None)
    point = P("gx", "gy", "gz", None, None)
    placed = (nodal,) * 3 + (point, P("gx", "gy", "gz", None, None, None)) + (point,) * 4
    return jax.shard_map(
        body, mesh=mesh, in_specs=placed, out_specs=(nodal,) * 3, check_vma=False
    )
```

```python
import functools

import jax
import jax.numpy as jnp
import numpy as np
from jax import lax
from jax.experimental import pallas as pl
from jax.experimental.pallas import tpu as pltpu
from jax.sharding import PartitionSpec as P

EX = 4
EY = 16
EZ = 2
NX = 4 * EX + 1
NY = 4 * EY + 1
NZ = 4 * EZ + 1
NODES = NX * NY * NZ
ROW = NY * NZ
XPAD = 24
FROWS = 960

time_step = 0.1
HALF = 0.5 * time_step
HALF_SQ = 0.5 * time_step * time_step
F32 = jnp.float32
BF16 = jnp.bfloat16
VMEM = pl.BlockSpec(memory_space=pltpu.VMEM)
HBM = pl.BlockSpec(memory_space=pltpu.HBM)


def derivative_table():
    points = np.array([-1.0, -np.sqrt(3.0 / 7.0), 0.0, np.sqrt(3.0 / 7.0), 1.0])
    count = points.shape[0]
    weights = np.array(
        [
            1.0 / np.prod([points[s] - points[o] for o in range(count) if o != s])
            for s in range(count)
        ]
    )
    table = np.zeros((count, count))
    for target in range(count):
        for source in range(count):
            if target != source:
                table[target, source] = (
                    weights[source] / weights[target] / (points[target] - points[source])
                )
        table[target, target] = -np.sum(table[target])
    return table


def operator_tables():
    table = derivative_table().astype(np.float32).astype(np.float64)
    eye = np.eye(5)
    full = np.zeros((3, 128, 128))
    full[0, :125, :125] = np.kron(np.kron(table, eye), eye)
    full[1, :125, :125] = np.kron(np.kron(eye, table), eye)
    full[2, :125, :125] = np.kron(np.kron(eye, eye), table)
    forward = full.reshape(384, 128)
    backward = -np.transpose(full, (2, 0, 1)).reshape(128, 384)
    out = []
    for matrix in (forward, backward):
        high = matrix.astype(np.float32).astype(jnp.bfloat16)
        low = (matrix - high.astype(np.float64)).astype(np.float32).astype(jnp.bfloat16)
        out.append((high, low))
    (forward_h, forward_l), (backward_h, backward_l) = out
    return (
        np.concatenate([forward_h, forward_l, forward_h], axis=1),
        np.concatenate([backward_h, backward_l], axis=0),
    )


def split(value):
    high = value.astype(BF16)
    return high, (value - high.astype(F32)).astype(BF16)


def dot(lhs, rhs):
    return lax.dot_general(lhs, rhs, (((1,), (0,)), ((), ())), preferred_element_type=F32)


def take(value, index):
    return jnp.take_along_axis(value, index, axis=1, mode="promise_in_bounds")


def lanes(shape=(8, 128)):
    return lax.broadcasted_iota(jnp.int32, shape, len(shape) - 1)


def force_kernel(
    d_hbm, v_hbm, a_hbm, n_hbm, m_hbm, j_hbm, l_hbm, s_hbm, r_hbm, fw_hbm, bw_hbm,
    t_ref, o_ref, y_ref, vh_ref, pos_s,
    d_s, v_s, a_s, n_s, m_s, j_s, l_s, s_s, r_s, fw_s, bw_s,
    grid_s, nodal_s, local_s, grad_s, fluxh_s, fluxl_s, sems,
):
    copies = []
    moves = [(n_hbm.at[pl.ds(0, 1)], n_s)]
    for src, dst in ((d_hbm, d_s), (v_hbm, v_s), (a_hbm, a_s)):
        moves += [(src.at[m], dst.at[m]) for m in range(3)]
    moves.append((fw_hbm, fw_s))
    for k in range(9):
        moves.append((m_hbm.at[pl.ds(125 * k, 125), 0], m_s.at[k, pl.ds(0, 125)]))
    for src, dst in ((j_hbm, j_s), (l_hbm, l_s), (s_hbm, s_s), (r_hbm, r_s)):
        moves.append((src.at[pl.ds(0, 125), 0], dst.at[pl.ds(0, 125)]))
    moves.append((bw_hbm, bw_s))
    for at, (src, dst) in enumerate(moves):
        copy = pltpu.make_async_copy(src, dst, sems.at[at])
        copy.start()
        copies.append(copy)
    for at in range(10):
        copies[at].wait()
    accel = a_s[...]
    veloc = v_s[...]
    pos_s[...] = d_s[...] + time_step * veloc + HALF_SQ * accel
    vh_ref[...] = veloc + HALF * accel
    lane = lanes()

    corner = jnp.broadcast_to(n_s[0], (8, 128))
    elem_x = (
        (corner >= 2340).astype(jnp.int32)
        + (corner >= 4680).astype(jnp.int32)
        + (corner >= 7020).astype(jnp.int32)
    )
    rest = corner - 2340 * elem_x
    elem_y = jnp.floor((rest.astype(F32) + 0.5) * (1.0 / 36.0)).astype(jnp.int32)
    elem_z = (rest - 36 * elem_y) >> 2
    group = elem_x * 2 + elem_z
    brick = (group * 16 + elem_y).astype(F32)
    column = jnp.broadcast_to(brick[0:1], (128, 128)).T
    hit = column == lanes((128, 128)).astype(F32)
    slot_index = lax.broadcasted_iota(jnp.int32, (128, 128), 0).astype(F32)
    slot_of = jnp.sum(jnp.where(hit, slot_index, 0.0), axis=0, keepdims=True)
    slot_of = jnp.broadcast_to(slot_of, (8, 128)).astype(jnp.int32)

    for m in range(3):
        for x in range(NX):
            value = pos_s[m, :, pl.ds(ROW * x, ROW)]
            if x < 16:
                grid_s[m, x : x + 1, :ROW] = value
            else:
                grid_s[3, m : m + 1, :ROW] = value
    places = [9 * (lane & 63) + 4 * (lane >> 6) + c for c in range(5)]
    for u in range(2):
        c = jnp.minimum(4 * u + (lane >> 5), 4)
        places.append(36 * (lane & 15) + 36 + c + 4 * ((lane >> 4) & 1))
    for m in range(4):
        for tile in range(2 if m < 3 else 1):
            rows = slice(8 * tile, 8 * tile + 8)
            parts = [grid_s[m, rows, 128 * v : 128 * v + 128] for v in range(5)]
            for c in range(7):
                low = places[c] & 127
                high = places[c] >> 7
                got = take(parts[0], low)
                for v in range(1, 5):
                    got = jnp.where(high == v, take(parts[v], low), got)
                if m < 3:
                    nodal_s[m, c, rows, :] = got
                else:
                    for k in range(3):
                        nodal_s[k, c, 16:17, :] = got[k : k + 1]

    masks = [elem_x == x for x in range(4)]
    inner = 64 * elem_z + 4 * elem_y
    outer = 16 * elem_z + elem_y
    for m in range(3):
        local_s[m, 120:128, :] = jnp.zeros((8, 128), F32)
        for c in range(5):
            near = [nodal_s[m, c, 4 * x : 4 * x + 8, :] for x in range(4)]
            last = [nodal_s[m, 5 + c // 4, 4 * x : 4 * x + 8, :] for x in range(4)]
            for b in range(5):
                parts, at = (near, inner + b) if b < 4 else (last, outer + 32 * (c % 4))
                got = take(parts[0], at)
                for x in range(1, 4):
                    got = jnp.where(masks[x], take(parts[x], at), got)
                local_s[m, pl.ds(5 * b + c, 5, stride=25), :] = got[:5]

    copies[10].wait()
    local = jnp.concatenate([local_s[m] for m in range(3)], axis=1)
    high, low = split(local)
    grad_s[...] = dot(fw_s[...], jnp.concatenate([high, high, low], axis=0))

    for at in range(11, 24):
        copies[at].wait()
    for chunk in range(8):
        at = 16 * chunk
        rows = slice(at, at + 16)
        g = [
            [grad_s[128 * l + at : 128 * l + at + 16, 128 * c : 128 * c + 128] for c in range(3)]
            for l in range(3)
        ]
        mp = [[m_s[3 * l + j, rows, :] for j in range(3)] for l in range(3)]
        gr = [
            [g[0][c] * mp[0][j] + g[1][c] * mp[1][j] + g[2][c] * mp[2][j] for j in range(3)]
            for c in range(3)
        ]
        mu = s_s[rows, :]
        trace = l_s[rows, :] * (gr[0][0] + gr[1][1] + gr[2][2])
        weight = j_s[rows, :]
        stress = [[None] * 3 for _ in range(3)]
        for c in range(3):
            for j in range(c, 3):
                value = mu * (gr[c][j] + gr[j][c])
                stress[c][j] = stress[j][c] = value + trace if c == j else value
        keep = lax.broadcasted_iota(jnp.int32, (16, 128), 0) < 125 - at
        mass = r_s[rows, :] * weight
        t_ref[3, rows, :] = jnp.where(keep, mass, 0.0) if chunk == 7 else mass
        for l in range(3):
            for c in range(3):
                flux = weight * (
                    stress[c][0] * mp[l][0] + stress[c][1] * mp[l][1] + stress[c][2] * mp[l][2]
                )
                if chunk == 7:
                    flux = jnp.where(keep, flux, 0.0)
                high, low = split(flux)
                to = slice(128 * l + at, 128 * l + at + 16)
                cols = slice(128 * c, 128 * c + 128)
                fluxh_s[to, cols] = high
                fluxl_s[to, cols] = low

    copies[24].wait()
    both = dot(bw_s[...], fluxh_s[...])
    terms = both[:128] + both[128:] + dot(bw_s[0:128, :], fluxl_s[...])
    for m in range(3):
        t_ref[m, 0:128, :] = terms[:, 128 * m : 128 * m + 128]
    for m in range(4):
        t_ref[m, 128:200, :] = jnp.zeros((72, 128), F32)
    o_ref[...] = slot_of

    edge = take(slot_of, 16 * (lane & 7) + 15 * ((lane >> 3) & 1))
    second = ((lane >> 3) & 1) == 1
    packs = []
    for q in range(3):
        pack = jnp.zeros((8, 128), F32)
        for k in range(8 * q, min(8 * q + 8, 20)):
            m, c = divmod(k, 5)
            got = jnp.where(
                second,
                take(t_ref[m, pl.ds(20 + c, 8, stride=25), :], edge),
                take(t_ref[m, pl.ds(c, 8, stride=25), :], edge),
            )
            pack = jnp.where((lane >> 4) == k - 8 * q, got, pack)
        packs.append(pack)
    even = 1 - lax.axis_index("gy") % 2
    upper = (lane >= 64).astype(jnp.int32)
    face = upper + even - 2 * upper * even
    plane = lane - 64 * upper
    comp = (
        (plane >= 9).astype(jnp.int32)
        + (plane >= 18).astype(jnp.int32)
        + (plane >= 27).astype(jnp.int32)
    )
    z = plane - 9 * comp
    row = lax.broadcasted_iota(jnp.int32, (8, 128), 0)
    zero = jnp.zeros((8, 128), F32)
    parts = []
    for x in range(4):
        total = zero
        for h in range(2):
            c = z - 4 * h
            good = (c >= 0) & (c <= 4) & (plane < 36)
            k = 5 * comp + c
            at = (16 * (k & 7) + 8 * face + 2 * x + h) & 127
            for q in range(3):
                total = total + jnp.where(good & ((k >> 3) == q), take(packs[q], at), zero)
        parts.append(total)
    stack_rows(parts, row, zero, y_ref, 0)


def stack_rows(parts, row, zero, out_ref, at):
    second = pltpu.roll(parts[1], 4, 0)
    fourth = pltpu.roll(parts[3], 4, 0)
    out_ref[at : at + 8, :] = parts[0] + jnp.where(row >= 4, second, zero)
    out_ref[at + 8 : at + 16, :] = (
        parts[2] + jnp.where(row < 4, second, zero) + jnp.where(row >= 4, fourth, zero)
    )
    out_ref[at + 16 : at + 24, :] = jnp.where(row < 4, fourth, zero)


def field_kernel(t_ref, o_ref, f_ref):
    slot_of = o_ref[...]
    lane = lanes()
    gathers = []
    for g in range(8):
        base = 16 * g + (lane >> 2)
        gathers.append(
            (take(slot_of, jnp.minimum(base, 127)), take(slot_of, jnp.clip(base - 1, 0, 127)))
        )
    quarter = lane & 3
    inside = lane < 64
    firsts = [(quarter == b) & inside for b in range(4)]
    lasts = (quarter == 0) & (lane >= 4) & (lane < 68)
    row = lax.broadcasted_iota(jnp.int32, (8, 128), 0)
    zero = jnp.zeros((8, 128), F32)
    for m in range(4):
        planes = {}
        for c in range(5):
            parts = [t_ref[m, pl.ds(5 * b + c, 8, stride=25), :] for b in range(5)]
            for g in range(8):
                at, before = gathers[g]
                got = jnp.where(firsts[0], take(parts[0], at), zero)
                for b in range(1, 4):
                    got = jnp.where(firsts[b], take(parts[b], at), got)
                got = got + jnp.where(lasts, take(parts[4], before), zero)
                key = (4 * (g % 2) + c, g // 2)
                planes[key] = planes[key] + got if key in planes else got
        for z in range(NZ):
            stack_rows([planes[(z, x)] for x in range(4)], row, zero, f_ref, (m * 9 + z) * XPAD)
    f_ref[36 * XPAD : FROWS, :] = jnp.zeros((FROWS - 36 * XPAD, 128), F32)


def y_faces(near, far):
    at = lax.axis_index("gy")
    odd = at % 2 == 1
    outer = (at > 0) & (at < lax.axis_size("gy") - 1)
    far = jnp.where(outer, far, 0.0)
    return jnp.where(odd, near, far), jnp.where(odd, far, near)


def x_kernel(y_ref, f_ref, xa_ref, xb_ref):
    pad = jnp.zeros((128 - XPAD, 128), F32)
    both = jnp.concatenate([y_ref[...], pad], axis=0).T
    lo, hi = y_faces(both[0:40], both[64:104])
    lane = lanes((40, 128))

    def face(x):
        return (
            f_ref[pl.ds(x, 40, stride=XPAD), :]
            + jnp.where(lane == 0, pltpu.roll(lo, (128 - x) % 128, 1) if x else lo, 0.0)
            + jnp.where(lane == 64, pltpu.roll(hi, 64 - x, 1), 0.0)
        )

    first = face(0)
    last = face(16)
    odd = lax.axis_index("gx") % 2 == 1
    xa_ref[...] = jnp.where(odd, first, last)
    xb_ref[...] = jnp.where(odd, last, first)


def y_kernel(y_ref, f_in, f_ref):
    lane = lanes()
    for tile in range(3):
        rows = slice(8 * tile, 8 * tile + 8)
        lo, hi = y_faces(y_ref[rows, :], pltpu.roll(y_ref[rows, :], 64, 1))
        for plane in range(36):
            to = slice(plane * XPAD + 8 * tile, plane * XPAD + 8 * tile + 8)
            low = pltpu.roll(lo, 128 - plane, 1) if plane else lo
            f_ref[to, :] = (
                f_in[to, :]
                + jnp.where(lane == 0, low, 0.0)
                + jnp.where(lane == 64, pltpu.roll(hi, (64 - plane) % 128, 1), 0.0)
            )


def z_kernel(xa_ref, xb_ref, f_in, f_ref, za_ref, zb_ref):
    at = lax.axis_index("gx")
    odd = at % 2 == 1
    outer = (at > 0) & (at < lax.axis_size("gx") - 1)
    near = xa_ref[0:36, :]
    far = jnp.where(outer, xb_ref[0:36, :], 0.0)
    f_ref[0 : 36 * XPAD, :] = f_in[0 : 36 * XPAD, :]
    f_ref[pl.ds(0, 36, stride=XPAD), :] = f_in[pl.ds(0, 36, stride=XPAD), :] + jnp.where(
        odd, near, far
    )
    f_ref[pl.ds(16, 36, stride=XPAD), :] = f_in[pl.ds(16, 36, stride=XPAD), :] + jnp.where(
        odd, far, near
    )
    odd = lax.axis_index("gz") % 2 == 1
    for m in range(4):
        at = m * 9 * XPAD
        first = f_ref[at : at + XPAD, :]
        last = f_ref[at + 8 * XPAD : at + 9 * XPAD, :]
        za_ref[XPAD * m : XPAD * m + XPAD, :] = jnp.where(odd, first, last)
        zb_ref[XPAD * m : XPAD * m + XPAD, :] = jnp.where(odd, last, first)


def row_spots(lane):
    spots = []
    for v in range(5):
        at = lane + 128 * v
        y = jnp.floor((at.astype(F32) + 0.5) * (1.0 / 9.0)).astype(jnp.int32)
        spots.append((y, at - 9 * y))
    return spots


def inner_kernel(f_ref, d_ref, grid_ref, d_out, acc_s, sem):
    out_copy = pltpu.make_async_copy(d_ref, d_out, sem)
    out_copy.start()
    for z in range(1, 8):
        for tile in range(3):
            rows = [(m * 9 + z) * XPAD + 8 * tile for m in range(4)]
            mass = f_ref[rows[3] : rows[3] + 8, :]
            for m in range(3):
                value = f_ref[rows[m] : rows[m] + 8, :] / mass
                if tile < 2:
                    acc_s[m, z, 8 * tile : 8 * tile + 8, :] = value
                else:
                    acc_s[3, z, m : m + 1, :] = value[0:1]
    spots = row_spots(lanes())
    for m in range(4):
        for tile in range(2 if m < 3 else 1):
            rows = slice(8 * tile, 8 * tile + 8)
            for v in range(5):
                y, z_of = spots[v]
                got = take(acc_s[m, 1, rows, :], y)
                for z in range(2, 8):
                    got = jnp.where(z_of == z, take(acc_s[m, z, rows, :], y), got)
                grid_ref[m, rows, 128 * v : 128 * v + 128] = got
    grid_ref[3, 8:16, :] = jnp.zeros((8, 640), F32)
    out_copy.wait()


def end_kernel(
    za_ref, zb_ref, f_ref, vh_ref, inner_ref, v_out, a_out, a_s, v_s, acc_s, grid_s, sems
):
    at = lax.axis_index("gz")
    odd = at % 2 == 1
    outer = (at > 0) & (at < lax.axis_size("gz") - 1)
    spots = row_spots(lanes())

    def added(m, z, tile):
        at = (m * 9 + z) * XPAD + 8 * tile
        rows = slice(XPAD * m + 8 * tile, XPAD * m + 8 * tile + 8)
        near = za_ref[rows, :]
        far = jnp.where(outer, zb_ref[rows, :], 0.0)
        return f_ref[at : at + 8, :] + (
            jnp.where(odd, near, far) if z == 0 else jnp.where(odd, far, near)
        )

    def to_rows(m, tile):
        rows = slice(8 * tile, 8 * tile + 8)
        for v in range(5):
            y, z_of = spots[v]
            cols = slice(128 * v, 128 * v + 128)
            got = jnp.where(z_of == 0, take(acc_s[m, 0, rows, :], y), inner_ref[m, rows, cols])
            got = jnp.where(z_of == 8, take(acc_s[m, 1, rows, :], y), got)
            grid_s[m, rows, cols] = got

    for z in (0, 8):
        for tile in range(3):
            mass = added(3, z, tile)
            for m in range(3):
                value = added(m, z, tile) / mass
                if tile < 2:
                    acc_s[m, z // 8, 8 * tile : 8 * tile + 8, :] = value
                else:
                    acc_s[3, z // 8, m : m + 1, :] = value[0:1]
    to_rows(3, 0)
    for m in range(3):
        to_rows(m, 0)
        to_rows(m, 1)
        for x in range(16):
            a_s[m, :, pl.ds(ROW * x, ROW)] = grid_s[m, x : x + 1, :ROW]
        a_s[m, :, pl.ds(ROW * 16, ROW)] = grid_s[3, m : m + 1, :ROW]
    a_copy = pltpu.make_async_copy(a_s, a_out, sems.at[0])
    a_copy.start()
    v_s[...] = vh_ref[...] + HALF * a_s[...]
    v_copy = pltpu.make_async_copy(v_s, v_out, sems.at[1])
    v_copy.start()
    a_copy.wait()
    v_copy.wait()


def swap(value, at, second):
    axes = ("gx", "gy", "gz")
    sizes = [lax.axis_size(axis) for axis in axes]
    other = 0 if at == 2 else 2
    pairs = []
    for index in np.ndindex(*sizes):
        target = list(index)
        if not second:
            target[at] ^= 1
        elif 0 < index[at] < sizes[at] - 1:
            target[at] = ((index[at] - 1) ^ 1) + 1
        else:
            target[other] ^= 1
        pairs.append(tuple(int(np.ravel_multi_index(i, sizes)) for i in (index, target)))
    return lax.ppermute(value, axes, pairs)


def body(displ, veloc, accel, node_index, inv_map, jac_weight, lame_first, shear_mod, density):
    f32 = functools.partial(jax.ShapeDtypeStruct, dtype=F32)
    flat = (3, 1, NODES)
    points = (125, 1, 128)
    tables = [jnp.asarray(table) for table in operator_tables()]
    scratch = [
        pltpu.VMEM(flat, F32), pltpu.VMEM(flat, F32), pltpu.VMEM(flat, F32),
        pltpu.VMEM((1, 1, 128), jnp.int32),
        pltpu.VMEM((9, 128, 128), F32),
        pltpu.VMEM((128, 128), F32), pltpu.VMEM((128, 128), F32),
        pltpu.VMEM((128, 128), F32), pltpu.VMEM((128, 128), F32),
        pltpu.VMEM((384, 384), BF16), pltpu.VMEM((256, 384), BF16),
        pltpu.VMEM((4, 16, 640), F32), pltpu.VMEM((3, 7, 24, 128), F32),
        pltpu.VMEM((3, 128, 128), F32), pltpu.VMEM((384, 384), F32),
        pltpu.VMEM((384, 384), BF16), pltpu.VMEM((384, 384), BF16),
        pltpu.SemaphoreType.DMA((25,)),
    ]
    terms, slots, ya, v_half, displ_new = pl.pallas_call(
        force_kernel,
        out_shape=(
            f32((4, 200, 128)), jax.ShapeDtypeStruct((8, 128), jnp.int32), f32((XPAD, 128)),
            f32(flat), f32(flat),
        ),
        in_specs=[HBM] * 11,
        out_specs=(VMEM,) * 5,
        scratch_shapes=scratch,
        compiler_params=pltpu.CompilerParams(vmem_limit_bytes=16 << 20),
    )(
        *(
            pltpu.with_memory_space_constraint(value, pltpu.HBM)
            for value in (
                displ.reshape(flat), veloc.reshape(flat), accel.reshape(flat),
                node_index.reshape(points), inv_map.reshape(1125, 1, 128),
                jac_weight.reshape(points), lame_first.reshape(points), shear_mod.reshape(points),
                density.reshape(points), *tables,
            )
        )
    )
    small = pltpu.CompilerParams(vmem_limit_bytes=8 << 20)
    count = lax.axis_size("gy")
    hops = [(i, (i - 2) % count if i % 2 == 0 else (i + 2) % count) for i in range(count)]
    passed = lax.ppermute(ya, "gy", hops)
    field = pl.pallas_call(
        field_kernel,
        out_shape=f32((FROWS, 128)),
        in_specs=[VMEM] * 2,
        out_specs=VMEM,
        compiler_params=small,
        cost_estimate=pl.CostEstimate(flops=4000000, bytes_accessed=800000, transcendentals=0),
    )(terms, slots)
    passed, field = lax.optimization_barrier((passed, field))
    ya = swap(jnp.where(lanes((XPAD, 128)) < 64, ya, passed), 1, False)
    face = f32((40, 128))
    xa, xb = pl.pallas_call(
        x_kernel,
        out_shape=(face, face),
        in_specs=[VMEM] * 2,
        out_specs=(VMEM,) * 2,
        compiler_params=small,
    )(ya, field)
    field = pl.pallas_call(
        y_kernel,
        out_shape=f32((FROWS, 128)),
        in_specs=[VMEM] * 2,
        out_specs=VMEM,
        input_output_aliases={1: 0},
        compiler_params=small,
        cost_estimate=pl.CostEstimate(flops=1000000, bytes_accessed=800000, transcendentals=0),
    )(ya, field)
    xa = swap(xa, 0, False)
    xb = swap(xb, 0, True)
    face = f32((96, 128))
    field, za, zb = pl.pallas_call(
        z_kernel,
        out_shape=(f32((FROWS, 128)), face, face),
        in_specs=[VMEM] * 3,
        out_specs=(VMEM,) * 3,
        input_output_aliases={2: 0},
        compiler_params=pltpu.CompilerParams(vmem_limit_bytes=8 << 20),
    )(xa, xb, field)
    za = swap(za, 2, False)
    zb = swap(zb, 2, True)
    inner, displ_out = pl.pallas_call(
        inner_kernel,
        out_shape=(f32((4, 16, 640)), f32(flat)),
        in_specs=[VMEM] * 2,
        out_specs=(VMEM, HBM),
        scratch_shapes=[pltpu.VMEM((4, 9, 16, 128), F32), pltpu.SemaphoreType.DMA],
        compiler_params=small,
        cost_estimate=pl.CostEstimate(flops=1000000, bytes_accessed=800000, transcendentals=0),
    )(field, displ_new)
    veloc_out, accel_out = pl.pallas_call(
        end_kernel,
        out_shape=(f32(flat), f32(flat)),
        in_specs=[VMEM] * 5,
        out_specs=(HBM, HBM),
        scratch_shapes=[
            pltpu.VMEM(flat, F32), pltpu.VMEM(flat, F32), pltpu.VMEM((4, 2, 16, 128), F32),
            pltpu.VMEM((4, 16, 640), F32), pltpu.SemaphoreType.DMA((2,)),
        ],
        compiler_params=pltpu.CompilerParams(vmem_limit_bytes=8 << 20),
    )(za, zb, field, v_half, inner)
    shape = (3, 1, 1, 1, NODES)
    return displ_out.reshape(shape), veloc_out.reshape(shape), accel_out.reshape(shape)


def solution(mesh):
    nodal = P(None, "gx", "gy", "gz", None)
    point = P("gx", "gy", "gz", None, None)
    placed = (nodal,) * 3 + (point, P("gx", "gy", "gz", None, None, None)) + (point,) * 4
    return jax.shard_map(
        body, mesh=mesh, in_specs=placed, out_specs=(nodal,) * 3, check_vma=False
    )
```

```python
import functools

import jax
import jax.numpy as jnp
import numpy as np
from jax import lax
from jax.experimental import pallas as pl
from jax.experimental.pallas import tpu as pltpu
from jax.sharding import PartitionSpec as P

EX = 4
EY = 16
EZ = 2
NX = 4 * EX + 1
NY = 4 * EY + 1
NZ = 4 * EZ + 1
NODES = NX * NY * NZ
ROW = NY * NZ
XPAD = 24
FROWS = 960

time_step = 0.1
HALF = 0.5 * time_step
HALF_SQ = 0.5 * time_step * time_step
F32 = jnp.float32
BF16 = jnp.bfloat16
VMEM = pl.BlockSpec(memory_space=pltpu.VMEM)
HBM = pl.BlockSpec(memory_space=pltpu.HBM)


def derivative_table():
    points = np.array([-1.0, -np.sqrt(3.0 / 7.0), 0.0, np.sqrt(3.0 / 7.0), 1.0])
    count = points.shape[0]
    weights = np.array(
        [
            1.0 / np.prod([points[s] - points[o] for o in range(count) if o != s])
            for s in range(count)
        ]
    )
    table = np.zeros((count, count))
    for target in range(count):
        for source in range(count):
            if target != source:
                table[target, source] = (
                    weights[source] / weights[target] / (points[target] - points[source])
                )
        table[target, target] = -np.sum(table[target])
    return table


def operator_tables():
    table = derivative_table().astype(np.float32).astype(np.float64)
    eye = np.eye(5)
    full = np.zeros((3, 128, 128))
    full[0, :125, :125] = np.kron(np.kron(table, eye), eye)
    full[1, :125, :125] = np.kron(np.kron(eye, table), eye)
    full[2, :125, :125] = np.kron(np.kron(eye, eye), table)
    forward = full.reshape(384, 128)
    backward = -np.transpose(full, (2, 0, 1)).reshape(128, 384)
    out = []
    for matrix in (forward, backward):
        high = matrix.astype(np.float32).astype(jnp.bfloat16)
        low = (matrix - high.astype(np.float64)).astype(np.float32).astype(jnp.bfloat16)
        out.append((high, low))
    (forward_h, forward_l), (backward_h, backward_l) = out
    return (
        np.concatenate([forward_h, forward_l, forward_h], axis=1),
        np.concatenate([backward_h, backward_l], axis=0),
    )


def split(value):
    high = value.astype(BF16)
    return high, (value - high.astype(F32)).astype(BF16)


def dot(lhs, rhs):
    return lax.dot_general(lhs, rhs, (((1,), (0,)), ((), ())), preferred_element_type=F32)


def take(value, index):
    return jnp.take_along_axis(value, index, axis=1, mode="promise_in_bounds")


def lanes(shape=(8, 128)):
    return lax.broadcasted_iota(jnp.int32, shape, len(shape) - 1)


def force_kernel(
    d_hbm, v_hbm, a_hbm, n_hbm, m_hbm, j_hbm, l_hbm, s_hbm, r_hbm, fw_hbm, bw_hbm,
    t_ref, o_ref, y_ref, v_s, a_s, pos_s,
    d_s, n_s, m_s, j_s, l_s, s_s, r_s, fw_s, bw_s,
    grid_s, nodal_s, local_s, grad_s, fluxh_s, fluxl_s, sems,
):
    copies = []
    moves = [(n_hbm.at[pl.ds(0, 1)], n_s)]
    for src, dst in ((d_hbm, d_s), (v_hbm, v_s), (a_hbm, a_s)):
        moves += [(src.at[m], dst.at[m]) for m in range(3)]
    moves.append((fw_hbm, fw_s))
    for k in range(9):
        moves.append((m_hbm.at[pl.ds(125 * k, 125), 0], m_s.at[k, pl.ds(0, 125)]))
    for src, dst in ((j_hbm, j_s), (l_hbm, l_s), (s_hbm, s_s), (r_hbm, r_s)):
        moves.append((src.at[pl.ds(0, 125), 0], dst.at[pl.ds(0, 125)]))
    moves.append((bw_hbm, bw_s))
    for at, (src, dst) in enumerate(moves):
        copy = pltpu.make_async_copy(src, dst, sems.at[at])
        copy.start()
        copies.append(copy)
    lane = lanes()
    for m in range(4):
        t_ref[m, 128:200, :] = jnp.zeros((72, 128), F32)
    for m in range(3):
        local_s[m, 120:128, :] = jnp.zeros((8, 128), F32)
    copies[0].wait()

    corner = jnp.broadcast_to(n_s[0], (8, 128))
    elem_x = (
        (corner >= 2340).astype(jnp.int32)
        + (corner >= 4680).astype(jnp.int32)
        + (corner >= 7020).astype(jnp.int32)
    )
    rest = corner - 2340 * elem_x
    elem_y = jnp.floor((rest.astype(F32) + 0.5) * (1.0 / 36.0)).astype(jnp.int32)
    elem_z = (rest - 36 * elem_y) >> 2
    group = elem_x * 2 + elem_z
    brick = (group * 16 + elem_y).astype(F32)
    column = jnp.broadcast_to(brick[0:1], (128, 128)).T
    hit = column == lanes((128, 128)).astype(F32)
    slot_index = lax.broadcasted_iota(jnp.int32, (128, 128), 0).astype(F32)
    slot_of = jnp.sum(jnp.where(hit, slot_index, 0.0), axis=0, keepdims=True)
    slot_of = jnp.broadcast_to(slot_of, (8, 128)).astype(jnp.int32)

    for at in range(1, 10):
        copies[at].wait()
    pos_s[...] = d_s[...] + time_step * v_s[...] + HALF_SQ * a_s[...]

    for m in range(3):
        for x in range(NX):
            value = pos_s[m, :, pl.ds(ROW * x, ROW)]
            if x < 16:
                grid_s[m, x : x + 1, :ROW] = value
            else:
                grid_s[3, m : m + 1, :ROW] = value
    places = [9 * (lane & 63) + 4 * (lane >> 6) + c for c in range(5)]
    for u in range(2):
        c = jnp.minimum(4 * u + (lane >> 5), 4)
        places.append(36 * (lane & 15) + 36 + c + 4 * ((lane >> 4) & 1))
    for m in range(4):
        for tile in range(2 if m < 3 else 1):
            rows = slice(8 * tile, 8 * tile + 8)
            parts = [grid_s[m, rows, 128 * v : 128 * v + 128] for v in range(5)]
            for c in range(7):
                low = places[c] & 127
                high = places[c] >> 7
                got = take(parts[0], low)
                for v in range(1, 5):
                    got = jnp.where(high == v, take(parts[v], low), got)
                if m < 3:
                    nodal_s[m, c, rows, :] = got
                else:
                    for k in range(3):
                        nodal_s[k, c, 16:17, :] = got[k : k + 1]

    masks = [elem_x == x for x in range(4)]
    inner = 64 * elem_z + 4 * elem_y
    outer = 16 * elem_z + elem_y
    for m in range(3):
        for c in range(5):
            near = [nodal_s[m, c, 4 * x : 4 * x + 8, :] for x in range(4)]
            last = [nodal_s[m, 5 + c // 4, 4 * x : 4 * x + 8, :] for x in range(4)]
            for b in range(5):
                parts, at = (near, inner + b) if b < 4 else (last, outer + 32 * (c % 4))
                got = take(parts[0], at)
                for x in range(1, 4):
                    got = jnp.where(masks[x], take(parts[x], at), got)
                local_s[m, pl.ds(5 * b + c, 5, stride=25), :] = got[:5]

    copies[10].wait()
    local = jnp.concatenate([local_s[m] for m in range(3)], axis=1)
    high, low = split(local)
    grad_s[...] = dot(fw_s[...], jnp.concatenate([high, high, low], axis=0))

    for at in range(11, 24):
        copies[at].wait()
    for chunk in range(8):
        at = 16 * chunk
        rows = slice(at, at + 16)
        g = [
            [grad_s[128 * l + at : 128 * l + at + 16, 128 * c : 128 * c + 128] for c in range(3)]
            for l in range(3)
        ]
        mp = [[m_s[3 * l + j, rows, :] for j in range(3)] for l in range(3)]
        gr = [
            [g[0][c] * mp[0][j] + g[1][c] * mp[1][j] + g[2][c] * mp[2][j] for j in range(3)]
            for c in range(3)
        ]
        mu = s_s[rows, :]
        trace = l_s[rows, :] * (gr[0][0] + gr[1][1] + gr[2][2])
        weight = j_s[rows, :]
        stress = [[None] * 3 for _ in range(3)]
        for c in range(3):
            for j in range(c, 3):
                value = mu * (gr[c][j] + gr[j][c])
                stress[c][j] = stress[j][c] = value + trace if c == j else value
        keep = lax.broadcasted_iota(jnp.int32, (16, 128), 0) < 125 - at
        mass = r_s[rows, :] * weight
        t_ref[3, rows, :] = jnp.where(keep, mass, 0.0) if chunk == 7 else mass
        for l in range(3):
            for c in range(3):
                flux = weight * (
                    stress[c][0] * mp[l][0] + stress[c][1] * mp[l][1] + stress[c][2] * mp[l][2]
                )
                if chunk == 7:
                    flux = jnp.where(keep, flux, 0.0)
                high, low = split(flux)
                to = slice(128 * l + at, 128 * l + at + 16)
                cols = slice(128 * c, 128 * c + 128)
                fluxh_s[to, cols] = high
                fluxl_s[to, cols] = low

    copies[24].wait()
    both = dot(bw_s[...], fluxh_s[...])
    terms = both[:128] + both[128:] + dot(bw_s[0:128, :], fluxl_s[...])
    for m in range(3):
        t_ref[m, 0:128, :] = terms[:, 128 * m : 128 * m + 128]
    o_ref[...] = slot_of

    edge = take(slot_of, 16 * (lane & 7) + 15 * ((lane >> 3) & 1))
    second = ((lane >> 3) & 1) == 1
    packs = []
    for q in range(3):
        pack = jnp.zeros((8, 128), F32)
        for k in range(8 * q, min(8 * q + 8, 20)):
            m, c = divmod(k, 5)
            got = jnp.where(
                second,
                take(t_ref[m, pl.ds(20 + c, 8, stride=25), :], edge),
                take(t_ref[m, pl.ds(c, 8, stride=25), :], edge),
            )
            pack = jnp.where((lane >> 4) == k - 8 * q, got, pack)
        packs.append(pack)
    even = 1 - lax.axis_index("gy") % 2
    upper = (lane >= 64).astype(jnp.int32)
    face = upper + even - 2 * upper * even
    plane = lane - 64 * upper
    comp = (
        (plane >= 9).astype(jnp.int32)
        + (plane >= 18).astype(jnp.int32)
        + (plane >= 27).astype(jnp.int32)
    )
    z = plane - 9 * comp
    row = lax.broadcasted_iota(jnp.int32, (8, 128), 0)
    zero = jnp.zeros((8, 128), F32)
    parts = []
    for x in range(4):
        total = zero
        for h in range(2):
            c = z - 4 * h
            good = (c >= 0) & (c <= 4) & (plane < 36)
            k = 5 * comp + c
            at = (16 * (k & 7) + 8 * face + 2 * x + h) & 127
            for q in range(3):
                total = total + jnp.where(good & ((k >> 3) == q), take(packs[q], at), zero)
        parts.append(total)
    stack_rows(parts, row, zero, y_ref, 0)


def stack_rows(parts, row, zero, out_ref, at):
    second = pltpu.roll(parts[1], 4, 0)
    fourth = pltpu.roll(parts[3], 4, 0)
    out_ref[at : at + 8, :] = parts[0] + jnp.where(row >= 4, second, zero)
    out_ref[at + 8 : at + 16, :] = (
        parts[2] + jnp.where(row < 4, second, zero) + jnp.where(row >= 4, fourth, zero)
    )
    out_ref[at + 16 : at + 24, :] = jnp.where(row < 4, fourth, zero)


def field_kernel(t_ref, o_ref, f_ref):
    slot_of = o_ref[...]
    lane = lanes()
    gathers = []
    for g in range(8):
        base = 16 * g + (lane >> 2)
        gathers.append(
            (take(slot_of, jnp.minimum(base, 127)), take(slot_of, jnp.clip(base - 1, 0, 127)))
        )
    quarter = lane & 3
    inside = lane < 64
    firsts = [(quarter == b) & inside for b in range(4)]
    lasts = (quarter == 0) & (lane >= 4) & (lane < 68)
    row = lax.broadcasted_iota(jnp.int32, (8, 128), 0)
    zero = jnp.zeros((8, 128), F32)
    for m in range(4):
        planes = {}
        for c in range(5):
            parts = [t_ref[m, pl.ds(5 * b + c, 8, stride=25), :] for b in range(5)]
            for g in range(8):
                at, before = gathers[g]
                got = jnp.where(firsts[0], take(parts[0], at), zero)
                for b in range(1, 4):
                    got = jnp.where(firsts[b], take(parts[b], at), got)
                got = got + jnp.where(lasts, take(parts[4], before), zero)
                key = (4 * (g % 2) + c, g // 2)
                planes[key] = planes[key] + got if key in planes else got
        for z in range(NZ):
            stack_rows([planes[(z, x)] for x in range(4)], row, zero, f_ref, (m * 9 + z) * XPAD)
    f_ref[36 * XPAD : FROWS, :] = jnp.zeros((FROWS - 36 * XPAD, 128), F32)


def y_faces(near, far):
    at = lax.axis_index("gy")
    odd = at % 2 == 1
    outer = (at > 0) & (at < lax.axis_size("gy") - 1)
    far = jnp.where(outer, far, 0.0)
    return jnp.where(odd, near, far), jnp.where(odd, far, near)


def x_kernel(y_ref, f_ref, xa_ref, xb_ref):
    pad = jnp.zeros((128 - XPAD, 128), F32)
    both = jnp.concatenate([y_ref[...], pad], axis=0).T
    lo, hi = y_faces(both[0:40], both[64:104])
    lane = lanes((40, 128))

    def face(x):
        return (
            f_ref[pl.ds(x, 40, stride=XPAD), :]
            + jnp.where(lane == 0, pltpu.roll(lo, (128 - x) % 128, 1) if x else lo, 0.0)
            + jnp.where(lane == 64, pltpu.roll(hi, 64 - x, 1), 0.0)
        )

    first = face(0)
    last = face(16)
    odd = lax.axis_index("gx") % 2 == 1
    xa_ref[...] = jnp.where(odd, first, last)
    xb_ref[...] = jnp.where(odd, last, first)


def y_kernel(y_ref, f_in, f_ref):
    lane = lanes()
    for tile in range(3):
        rows = slice(8 * tile, 8 * tile + 8)
        lo, hi = y_faces(y_ref[rows, :], pltpu.roll(y_ref[rows, :], 64, 1))
        for plane in range(36):
            to = slice(plane * XPAD + 8 * tile, plane * XPAD + 8 * tile + 8)
            low = pltpu.roll(lo, 128 - plane, 1) if plane else lo
            f_ref[to, :] = (
                f_in[to, :]
                + jnp.where(lane == 0, low, 0.0)
                + jnp.where(lane == 64, pltpu.roll(hi, (64 - plane) % 128, 1), 0.0)
            )


def z_kernel(xa_ref, xb_ref, f_in, f_ref, za_ref, zb_ref):
    at = lax.axis_index("gx")
    odd = at % 2 == 1
    outer = (at > 0) & (at < lax.axis_size("gx") - 1)
    near = xa_ref[0:36, :]
    far = jnp.where(outer, xb_ref[0:36, :], 0.0)
    f_ref[0 : 36 * XPAD, :] = f_in[0 : 36 * XPAD, :]
    f_ref[pl.ds(0, 36, stride=XPAD), :] = f_in[pl.ds(0, 36, stride=XPAD), :] + jnp.where(
        odd, near, far
    )
    f_ref[pl.ds(16, 36, stride=XPAD), :] = f_in[pl.ds(16, 36, stride=XPAD), :] + jnp.where(
        odd, far, near
    )
    odd = lax.axis_index("gz") % 2 == 1
    for m in range(4):
        at = m * 9 * XPAD
        first = f_ref[at : at + XPAD, :]
        last = f_ref[at + 8 * XPAD : at + 9 * XPAD, :]
        za_ref[XPAD * m : XPAD * m + XPAD, :] = jnp.where(odd, first, last)
        zb_ref[XPAD * m : XPAD * m + XPAD, :] = jnp.where(odd, last, first)


def row_spots(lane):
    spots = []
    for v in range(5):
        at = lane + 128 * v
        y = jnp.floor((at.astype(F32) + 0.5) * (1.0 / 9.0)).astype(jnp.int32)
        spots.append((y, at - 9 * y))
    return spots


def inner_kernel(f_ref, d_ref, v_ref, a_ref, grid_ref, vh_ref, d_out, acc_s, sem):
    out_copy = pltpu.make_async_copy(d_ref, d_out, sem)
    out_copy.start()
    vh_ref[...] = v_ref[...] + HALF * a_ref[...]
    for z in range(1, 8):
        for tile in range(3):
            rows = [(m * 9 + z) * XPAD + 8 * tile for m in range(4)]
            mass = f_ref[rows[3] : rows[3] + 8, :]
            for m in range(3):
                value = f_ref[rows[m] : rows[m] + 8, :] / mass
                if tile < 2:
                    acc_s[m, z, 8 * tile : 8 * tile + 8, :] = value
                else:
                    acc_s[3, z, m : m + 1, :] = value[0:1]
    spots = row_spots(lanes())
    for m in range(4):
        for tile in range(2 if m < 3 else 1):
            rows = slice(8 * tile, 8 * tile + 8)
            for v in range(5):
                y, z_of = spots[v]
                got = take(acc_s[m, 1, rows, :], y)
                for z in range(2, 8):
                    got = jnp.where(z_of == z, take(acc_s[m, z, rows, :], y), got)
                grid_ref[m, rows, 128 * v : 128 * v + 128] = got
    grid_ref[3, 8:16, :] = jnp.zeros((8, 640), F32)
    out_copy.wait()


def end_kernel(
    za_ref, zb_ref, f_ref, vh_ref, inner_ref, v_out, a_out, a_s, v_s, acc_s, grid_s, sems
):
    at = lax.axis_index("gz")
    odd = at % 2 == 1
    outer = (at > 0) & (at < lax.axis_size("gz") - 1)
    spots = row_spots(lanes())

    def added(m, z, tile):
        at = (m * 9 + z) * XPAD + 8 * tile
        rows = slice(XPAD * m + 8 * tile, XPAD * m + 8 * tile + 8)
        near = za_ref[rows, :]
        far = jnp.where(outer, zb_ref[rows, :], 0.0)
        return f_ref[at : at + 8, :] + (
            jnp.where(odd, near, far) if z == 0 else jnp.where(odd, far, near)
        )

    def to_rows(m, tile):
        rows = slice(8 * tile, 8 * tile + 8)
        for v in range(5):
            y, z_of = spots[v]
            cols = slice(128 * v, 128 * v + 128)
            got = jnp.where(z_of == 0, take(acc_s[m, 0, rows, :], y), inner_ref[m, rows, cols])
            got = jnp.where(z_of == 8, take(acc_s[m, 1, rows, :], y), got)
            grid_s[m, rows, cols] = got

    for z in (0, 8):
        for tile in range(3):
            mass = added(3, z, tile)
            for m in range(3):
                value = added(m, z, tile) / mass
                if tile < 2:
                    acc_s[m, z // 8, 8 * tile : 8 * tile + 8, :] = value
                else:
                    acc_s[3, z // 8, m : m + 1, :] = value[0:1]
    to_rows(3, 0)
    for m in range(3):
        to_rows(m, 0)
        to_rows(m, 1)
        for x in range(16):
            a_s[m, :, pl.ds(ROW * x, ROW)] = grid_s[m, x : x + 1, :ROW]
        a_s[m, :, pl.ds(ROW * 16, ROW)] = grid_s[3, m : m + 1, :ROW]
    a_copy = pltpu.make_async_copy(a_s, a_out, sems.at[0])
    a_copy.start()
    v_s[...] = vh_ref[...] + HALF * a_s[...]
    v_copy = pltpu.make_async_copy(v_s, v_out, sems.at[1])
    v_copy.start()
    a_copy.wait()
    v_copy.wait()


def swap(value, at, second):
    axes = ("gx", "gy", "gz")
    sizes = [lax.axis_size(axis) for axis in axes]
    other = 0 if at == 2 else 2
    pairs = []
    for index in np.ndindex(*sizes):
        target = list(index)
        if not second:
            target[at] ^= 1
        elif 0 < index[at] < sizes[at] - 1:
            target[at] = ((index[at] - 1) ^ 1) + 1
        else:
            target[other] ^= 1
        pairs.append(tuple(int(np.ravel_multi_index(i, sizes)) for i in (index, target)))
    return lax.ppermute(value, axes, pairs)


def body(displ, veloc, accel, node_index, inv_map, jac_weight, lame_first, shear_mod, density):
    f32 = functools.partial(jax.ShapeDtypeStruct, dtype=F32)
    flat = (3, 1, NODES)
    points = (125, 1, 128)
    tables = [jnp.asarray(table) for table in operator_tables()]
    scratch = [
        pltpu.VMEM(flat, F32), pltpu.VMEM((1, 1, 128), jnp.int32),
        pltpu.VMEM((9, 128, 128), F32),
        pltpu.VMEM((128, 128), F32), pltpu.VMEM((128, 128), F32),
        pltpu.VMEM((128, 128), F32), pltpu.VMEM((128, 128), F32),
        pltpu.VMEM((384, 384), BF16), pltpu.VMEM((256, 384), BF16),
        pltpu.VMEM((4, 16, 640), F32), pltpu.VMEM((3, 7, 24, 128), F32),
        pltpu.VMEM((3, 128, 128), F32), pltpu.VMEM((384, 384), F32),
        pltpu.VMEM((384, 384), BF16), pltpu.VMEM((384, 384), BF16),
        pltpu.SemaphoreType.DMA((25,)),
    ]
    terms, slots, ya, v_old, a_old, displ_new = pl.pallas_call(
        force_kernel,
        out_shape=(
            f32((4, 200, 128)), jax.ShapeDtypeStruct((8, 128), jnp.int32), f32((XPAD, 128)),
            f32(flat), f32(flat), f32(flat),
        ),
        in_specs=[HBM] * 11,
        out_specs=(VMEM,) * 6,
        scratch_shapes=scratch,
        compiler_params=pltpu.CompilerParams(vmem_limit_bytes=16 << 20),
    )(
        *(
            pltpu.with_memory_space_constraint(value, pltpu.HBM)
            for value in (
                displ.reshape(flat), veloc.reshape(flat), accel.reshape(flat),
                node_index.reshape(points), inv_map.reshape(1125, 1, 128),
                jac_weight.reshape(points), lame_first.reshape(points), shear_mod.reshape(points),
                density.reshape(points), *tables,
            )
        )
    )
    small = pltpu.CompilerParams(vmem_limit_bytes=8 << 20)
    count = lax.axis_size("gy")
    hops = [(i, (i - 2) % count if i % 2 == 0 else (i + 2) % count) for i in range(count)]
    passed = lax.ppermute(ya, "gy", hops)
    field = pl.pallas_call(
        field_kernel,
        out_shape=f32((FROWS, 128)),
        in_specs=[VMEM] * 2,
        out_specs=VMEM,
        compiler_params=small,
        cost_estimate=pl.CostEstimate(flops=4000000, bytes_accessed=800000, transcendentals=0),
    )(terms, slots)
    passed, field = lax.optimization_barrier((passed, field))
    ya = swap(jnp.where(lanes((XPAD, 128)) < 64, ya, passed), 1, False)
    face = f32((40, 128))
    xa, xb = pl.pallas_call(
        x_kernel,
        out_shape=(face, face),
        in_specs=[VMEM] * 2,
        out_specs=(VMEM,) * 2,
        compiler_params=small,
    )(ya, field)
    field = pl.pallas_call(
        y_kernel,
        out_shape=f32((FROWS, 128)),
        in_specs=[VMEM] * 2,
        out_specs=VMEM,
        input_output_aliases={1: 0},
        compiler_params=small,
        cost_estimate=pl.CostEstimate(flops=1000000, bytes_accessed=800000, transcendentals=0),
    )(ya, field)
    xa = swap(xa, 0, False)
    xb = swap(xb, 0, True)
    face = f32((96, 128))
    field, za, zb = pl.pallas_call(
        z_kernel,
        out_shape=(f32((FROWS, 128)), face, face),
        in_specs=[VMEM] * 3,
        out_specs=(VMEM,) * 3,
        input_output_aliases={2: 0},
        compiler_params=pltpu.CompilerParams(vmem_limit_bytes=8 << 20),
    )(xa, xb, field)
    za = swap(za, 2, False)
    zb = swap(zb, 2, True)
    inner, v_half, displ_out = pl.pallas_call(
        inner_kernel,
        out_shape=(f32((4, 16, 640)), f32(flat), f32(flat)),
        in_specs=[VMEM] * 4,
        out_specs=(VMEM, VMEM, HBM),
        scratch_shapes=[pltpu.VMEM((4, 9, 16, 128), F32), pltpu.SemaphoreType.DMA],
        compiler_params=small,
        cost_estimate=pl.CostEstimate(flops=1000000, bytes_accessed=800000, transcendentals=0),
    )(field, displ_new, v_old, a_old)
    veloc_out, accel_out = pl.pallas_call(
        end_kernel,
        out_shape=(f32(flat), f32(flat)),
        in_specs=[VMEM] * 5,
        out_specs=(HBM, HBM),
        scratch_shapes=[
            pltpu.VMEM(flat, F32), pltpu.VMEM(flat, F32), pltpu.VMEM((4, 2, 16, 128), F32),
            pltpu.VMEM((4, 16, 640), F32), pltpu.SemaphoreType.DMA((2,)),
        ],
        compiler_params=pltpu.CompilerParams(vmem_limit_bytes=8 << 20),
    )(za, zb, field, v_half, inner)
    shape = (3, 1, 1, 1, NODES)
    return displ_out.reshape(shape), veloc_out.reshape(shape), accel_out.reshape(shape)


def solution(mesh):
    nodal = P(None, "gx", "gy", "gz", None)
    point = P("gx", "gy", "gz", None, None)
    placed = (nodal,) * 3 + (point, P("gx", "gy", "gz", None, None, None)) + (point,) * 4
    return jax.shard_map(
        body, mesh=mesh, in_specs=placed, out_specs=(nodal,) * 3, check_vma=False
    )
```

```python
import functools

import jax
import jax.numpy as jnp
import numpy as np
from jax import lax
from jax.experimental import pallas as pl
from jax.experimental.pallas import tpu as pltpu
from jax.sharding import PartitionSpec as P

EX = 4
EY = 16
EZ = 2
NX = 4 * EX + 1
NY = 4 * EY + 1
NZ = 4 * EZ + 1
NODES = NX * NY * NZ
ROW = NY * NZ
XPAD = 24
FROWS = 960

time_step = 0.1
HALF = 0.5 * time_step
HALF_SQ = 0.5 * time_step * time_step
F32 = jnp.float32
BF16 = jnp.bfloat16
VMEM = pl.BlockSpec(memory_space=pltpu.VMEM)
HBM = pl.BlockSpec(memory_space=pltpu.HBM)


def derivative_table():
    points = np.array([-1.0, -np.sqrt(3.0 / 7.0), 0.0, np.sqrt(3.0 / 7.0), 1.0])
    count = points.shape[0]
    weights = np.array(
        [
            1.0 / np.prod([points[s] - points[o] for o in range(count) if o != s])
            for s in range(count)
        ]
    )
    table = np.zeros((count, count))
    for target in range(count):
        for source in range(count):
            if target != source:
                table[target, source] = (
                    weights[source] / weights[target] / (points[target] - points[source])
                )
        table[target, target] = -np.sum(table[target])
    return table


def operator_tables():
    table = derivative_table().astype(np.float32).astype(np.float64)
    eye = np.eye(5)
    full = np.zeros((3, 128, 128))
    full[0, :125, :125] = np.kron(np.kron(table, eye), eye)
    full[1, :125, :125] = np.kron(np.kron(eye, table), eye)
    full[2, :125, :125] = np.kron(np.kron(eye, eye), table)
    forward = full.reshape(384, 128)
    backward = -np.transpose(full, (2, 0, 1)).reshape(128, 384)
    out = []
    for matrix in (forward, backward):
        high = matrix.astype(np.float32).astype(jnp.bfloat16)
        low = (matrix - high.astype(np.float64)).astype(np.float32).astype(jnp.bfloat16)
        out.append((high, low))
    (forward_h, forward_l), (backward_h, backward_l) = out
    return (
        np.concatenate([forward_h, forward_l, forward_h], axis=1),
        np.concatenate([backward_h, backward_l], axis=0),
    )


def split(value):
    high = value.astype(BF16)
    return high, (value - high.astype(F32)).astype(BF16)


def dot(lhs, rhs):
    return lax.dot_general(lhs, rhs, (((1,), (0,)), ((), ())), preferred_element_type=F32)


def take(value, index):
    return jnp.take_along_axis(value, index, axis=1, mode="promise_in_bounds")


def lanes(shape=(8, 128)):
    return lax.broadcasted_iota(jnp.int32, shape, len(shape) - 1)


def force_kernel(
    d_hbm, v_hbm, a_hbm, n_hbm, m_hbm, j_hbm, l_hbm, s_hbm, r_hbm, fw_hbm, bw_hbm,
    t_ref, o_ref, y_ref, v_s, a_s, pos_s,
    d_s, n_s, m_s, j_s, l_s, s_s, r_s, fw_s, bw_s,
    grid_s, nodal_s, local_s, grad_s, wide_s, fluxh_s, fluxl_s, sems,
):
    copies = []
    moves = [(n_hbm.at[pl.ds(0, 1)], n_s)]
    for src, dst in ((d_hbm, d_s), (v_hbm, v_s), (a_hbm, a_s)):
        moves += [(src.at[m], dst.at[m]) for m in range(3)]
    moves.append((fw_hbm, fw_s))
    for k in range(9):
        moves.append((m_hbm.at[pl.ds(125 * k, 125), 0], m_s.at[k, pl.ds(0, 125)]))
    for src, dst in ((j_hbm, j_s), (l_hbm, l_s), (s_hbm, s_s), (r_hbm, r_s)):
        moves.append((src.at[pl.ds(0, 125), 0], dst.at[pl.ds(0, 125)]))
    moves.append((bw_hbm, bw_s))
    for at, (src, dst) in enumerate(moves):
        copy = pltpu.make_async_copy(src, dst, sems.at[at])
        copy.start()
        copies.append(copy)
    lane = lanes()
    for m in range(4):
        t_ref[m, 128:200, :] = jnp.zeros((72, 128), F32)
    for m in range(3):
        local_s[m, 120:128, :] = jnp.zeros((8, 128), F32)
    copies[0].wait()

    corner = jnp.broadcast_to(n_s[0], (8, 128))
    elem_x = (
        (corner >= 2340).astype(jnp.int32)
        + (corner >= 4680).astype(jnp.int32)
        + (corner >= 7020).astype(jnp.int32)
    )
    rest = corner - 2340 * elem_x
    elem_y = jnp.floor((rest.astype(F32) + 0.5) * (1.0 / 36.0)).astype(jnp.int32)
    elem_z = (rest - 36 * elem_y) >> 2
    group = elem_x * 2 + elem_z
    brick = (group * 16 + elem_y).astype(F32)
    column = jnp.broadcast_to(brick[0:1], (128, 128)).T
    hit = column == lanes((128, 128)).astype(F32)
    slot_index = lax.broadcasted_iota(jnp.int32, (128, 128), 0).astype(F32)
    slot_of = jnp.sum(jnp.where(hit, slot_index, 0.0), axis=0, keepdims=True)
    slot_of = jnp.broadcast_to(slot_of, (8, 128)).astype(jnp.int32)

    for at in range(1, 10):
        copies[at].wait()
    moved = d_s[...] + time_step * v_s[...] + HALF_SQ * a_s[...]
    pos_s[...] = moved
    wide_s[0:3] = moved

    for m in range(3):
        for x in range(NX):
            value = wide_s[m, :, pl.ds(ROW * x, ROW)]
            if x < 16:
                grid_s[m, x : x + 1, :ROW] = value
            else:
                grid_s[3, m : m + 1, :ROW] = value
    places = [9 * (lane & 63) + 4 * (lane >> 6) + c for c in range(5)]
    for u in range(2):
        c = jnp.minimum(4 * u + (lane >> 5), 4)
        places.append(36 * (lane & 15) + 36 + c + 4 * ((lane >> 4) & 1))
    for m in range(4):
        for tile in range(2 if m < 3 else 1):
            rows = slice(8 * tile, 8 * tile + 8)
            parts = [grid_s[m, rows, 128 * v : 128 * v + 128] for v in range(5)]
            for c in range(7):
                low = places[c] & 127
                high = places[c] >> 7
                got = take(parts[0], low)
                for v in range(1, 5):
                    got = jnp.where(high == v, take(parts[v], low), got)
                if m < 3:
                    nodal_s[m, c, rows, :] = got
                else:
                    for k in range(3):
                        nodal_s[k, c, 16:17, :] = got[k : k + 1]

    masks = [elem_x == x for x in range(4)]
    inner = 64 * elem_z + 4 * elem_y
    outer = 16 * elem_z + elem_y
    for m in range(3):
        for c in range(5):
            near = [nodal_s[m, c, 4 * x : 4 * x + 8, :] for x in range(4)]
            last = [nodal_s[m, 5 + c // 4, 4 * x : 4 * x + 8, :] for x in range(4)]
            for b in range(5):
                parts, at = (near, inner + b) if b < 4 else (last, outer + 32 * (c % 4))
                got = take(parts[0], at)
                for x in range(1, 4):
                    got = jnp.where(masks[x], take(parts[x], at), got)
                local_s[m, pl.ds(5 * b + c, 5, stride=25), :] = got[:5]

    copies[10].wait()
    local = jnp.concatenate([local_s[m, 0:128, :] for m in range(3)], axis=1)
    high, low = split(local)
    grad_s[...] = dot(fw_s[...], jnp.concatenate([high, high, low], axis=0))

    for at in range(11, 24):
        copies[at].wait()
    for chunk in range(8):
        at = 16 * chunk
        rows = slice(at, at + 16)
        g = [
            [grad_s[128 * l + at : 128 * l + at + 16, 128 * c : 128 * c + 128] for c in range(3)]
            for l in range(3)
        ]
        mp = [[m_s[3 * l + j, rows, :] for j in range(3)] for l in range(3)]
        gr = [
            [g[0][c] * mp[0][j] + g[1][c] * mp[1][j] + g[2][c] * mp[2][j] for j in range(3)]
            for c in range(3)
        ]
        mu = s_s[rows, :]
        trace = l_s[rows, :] * (gr[0][0] + gr[1][1] + gr[2][2])
        weight = j_s[rows, :]
        stress = [[None] * 3 for _ in range(3)]
        for c in range(3):
            for j in range(c, 3):
                value = mu * (gr[c][j] + gr[j][c])
                stress[c][j] = stress[j][c] = value + trace if c == j else value
        keep = lax.broadcasted_iota(jnp.int32, (16, 128), 0) < 125 - at
        mass = r_s[rows, :] * weight
        t_ref[3, rows, :] = jnp.where(keep, mass, 0.0) if chunk == 7 else mass
        for l in range(3):
            for c in range(3):
                flux = weight * (
                    stress[c][0] * mp[l][0] + stress[c][1] * mp[l][1] + stress[c][2] * mp[l][2]
                )
                if chunk == 7:
                    flux = jnp.where(keep, flux, 0.0)
                high, low = split(flux)
                to = slice(128 * l + at, 128 * l + at + 16)
                cols = slice(128 * c, 128 * c + 128)
                fluxh_s[to, cols] = high
                fluxl_s[to, cols] = low

    copies[24].wait()
    both = dot(bw_s[...], fluxh_s[...])
    terms = both[:128] + both[128:] + dot(bw_s[0:128, :], fluxl_s[...])
    for m in range(3):
        t_ref[m, 0:128, :] = terms[:, 128 * m : 128 * m + 128]
    o_ref[...] = slot_of

    edge = take(slot_of, 16 * (lane & 7) + 15 * ((lane >> 3) & 1))
    second = ((lane >> 3) & 1) == 1
    packs = []
    for q in range(3):
        pack = jnp.zeros((8, 128), F32)
        for k in range(8 * q, min(8 * q + 8, 20)):
            m, c = divmod(k, 5)
            got = jnp.where(
                second,
                take(t_ref[m, pl.ds(20 + c, 8, stride=25), :], edge),
                take(t_ref[m, pl.ds(c, 8, stride=25), :], edge),
            )
            pack = jnp.where((lane >> 4) == k - 8 * q, got, pack)
        packs.append(pack)
    even = 1 - lax.axis_index("gy") % 2
    upper = (lane >= 64).astype(jnp.int32)
    face = upper + even - 2 * upper * even
    plane = lane - 64 * upper
    comp = (
        (plane >= 9).astype(jnp.int32)
        + (plane >= 18).astype(jnp.int32)
        + (plane >= 27).astype(jnp.int32)
    )
    z = plane - 9 * comp
    row = lax.broadcasted_iota(jnp.int32, (8, 128), 0)
    zero = jnp.zeros((8, 128), F32)
    parts = []
    for x in range(4):
        total = zero
        for h in range(2):
            c = z - 4 * h
            good = (c >= 0) & (c <= 4) & (plane < 36)
            k = 5 * comp + c
            at = (16 * (k & 7) + 8 * face + 2 * x + h) & 127
            for q in range(3):
                total = total + jnp.where(good & ((k >> 3) == q), take(packs[q], at), zero)
        parts.append(total)
    stack_rows(parts, row, zero, y_ref, 0)


def stack_rows(parts, row, zero, out_ref, at):
    second = pltpu.roll(parts[1], 4, 0)
    fourth = pltpu.roll(parts[3], 4, 0)
    out_ref[at : at + 8, :] = parts[0] + jnp.where(row >= 4, second, zero)
    out_ref[at + 8 : at + 16, :] = (
        parts[2] + jnp.where(row < 4, second, zero) + jnp.where(row >= 4, fourth, zero)
    )
    out_ref[at + 16 : at + 24, :] = jnp.where(row < 4, fourth, zero)


def field_kernel(t_ref, o_ref, f_ref):
    slot_of = o_ref[...]
    lane = lanes()
    gathers = []
    for g in range(8):
        base = 16 * g + (lane >> 2)
        gathers.append(
            (take(slot_of, jnp.minimum(base, 127)), take(slot_of, jnp.clip(base - 1, 0, 127)))
        )
    quarter = lane & 3
    inside = lane < 64
    firsts = [(quarter == b) & inside for b in range(4)]
    lasts = (quarter == 0) & (lane >= 4) & (lane < 68)
    row = lax.broadcasted_iota(jnp.int32, (8, 128), 0)
    zero = jnp.zeros((8, 128), F32)
    for m in range(4):
        planes = {}
        for c in range(5):
            parts = [t_ref[m, pl.ds(5 * b + c, 8, stride=25), :] for b in range(5)]
            for g in range(8):
                at, before = gathers[g]
                got = jnp.where(firsts[0], take(parts[0], at), zero)
                for b in range(1, 4):
                    got = jnp.where(firsts[b], take(parts[b], at), got)
                got = got + jnp.where(lasts, take(parts[4], before), zero)
                key = (4 * (g % 2) + c, g // 2)
                planes[key] = planes[key] + got if key in planes else got
        for z in range(NZ):
            stack_rows([planes[(z, x)] for x in range(4)], row, zero, f_ref, (m * 9 + z) * XPAD)
    f_ref[36 * XPAD : FROWS, :] = jnp.zeros((FROWS - 36 * XPAD, 128), F32)


def y_faces(near, far):
    at = lax.axis_index("gy")
    odd = at % 2 == 1
    outer = (at > 0) & (at < lax.axis_size("gy") - 1)
    far = jnp.where(outer, far, 0.0)
    return jnp.where(odd, near, far), jnp.where(odd, far, near)


def x_kernel(y_ref, f_ref, xa_ref, xb_ref):
    pad = jnp.zeros((128 - XPAD, 128), F32)
    both = jnp.concatenate([y_ref[...], pad], axis=0).T
    lo, hi = y_faces(both[0:40], both[64:104])
    lane = lanes((40, 128))

    def face(x):
        return (
            f_ref[pl.ds(x, 40, stride=XPAD), :]
            + jnp.where(lane == 0, pltpu.roll(lo, (128 - x) % 128, 1) if x else lo, 0.0)
            + jnp.where(lane == 64, pltpu.roll(hi, 64 - x, 1), 0.0)
        )

    first = face(0)
    last = face(16)
    odd = lax.axis_index("gx") % 2 == 1
    xa_ref[...] = jnp.where(odd, first, last)
    xb_ref[...] = jnp.where(odd, last, first)


def y_kernel(y_ref, f_in, f_ref):
    lane = lanes()
    for tile in range(3):
        rows = slice(8 * tile, 8 * tile + 8)
        lo, hi = y_faces(y_ref[rows, :], pltpu.roll(y_ref[rows, :], 64, 1))
        for plane in range(36):
            to = slice(plane * XPAD + 8 * tile, plane * XPAD + 8 * tile + 8)
            low = pltpu.roll(lo, 128 - plane, 1) if plane else lo
            f_ref[to, :] = (
                f_in[to, :]
                + jnp.where(lane == 0, low, 0.0)
                + jnp.where(lane == 64, pltpu.roll(hi, (64 - plane) % 128, 1), 0.0)
            )


def z_kernel(xa_ref, xb_ref, f_in, f_ref, za_ref, zb_ref):
    at = lax.axis_index("gx")
    odd = at % 2 == 1
    outer = (at > 0) & (at < lax.axis_size("gx") - 1)
    near = xa_ref[0:36, :]
    far = jnp.where(outer, xb_ref[0:36, :], 0.0)
    f_ref[0 : 36 * XPAD, :] = f_in[0 : 36 * XPAD, :]
    f_ref[pl.ds(0, 36, stride=XPAD), :] = f_in[pl.ds(0, 36, stride=XPAD), :] + jnp.where(
        odd, near, far
    )
    f_ref[pl.ds(16, 36, stride=XPAD), :] = f_in[pl.ds(16, 36, stride=XPAD), :] + jnp.where(
        odd, far, near
    )
    odd = lax.axis_index("gz") % 2 == 1
    for m in range(4):
        at = m * 9 * XPAD
        first = f_ref[at : at + XPAD, :]
        last = f_ref[at + 8 * XPAD : at + 9 * XPAD, :]
        za_ref[XPAD * m : XPAD * m + XPAD, :] = jnp.where(odd, first, last)
        zb_ref[XPAD * m : XPAD * m + XPAD, :] = jnp.where(odd, last, first)


def row_spots(lane):
    spots = []
    for v in range(5):
        at = lane + 128 * v
        y = jnp.floor((at.astype(F32) + 0.5) * (1.0 / 9.0)).astype(jnp.int32)
        spots.append((y, at - 9 * y))
    return spots


def inner_kernel(f_ref, d_ref, v_ref, a_ref, grid_ref, vh_ref, d_out, acc_s, sem):
    out_copy = pltpu.make_async_copy(d_ref, d_out, sem)
    out_copy.start()
    vh_ref[...] = v_ref[...] + HALF * a_ref[...]
    for z in range(1, 8):
        for tile in range(3):
            rows = [(m * 9 + z) * XPAD + 8 * tile for m in range(4)]
            mass = f_ref[rows[3] : rows[3] + 8, :]
            for m in range(3):
                value = f_ref[rows[m] : rows[m] + 8, :] / mass
                if tile < 2:
                    acc_s[m, z, 8 * tile : 8 * tile + 8, :] = value
                else:
                    acc_s[3, z, m : m + 1, :] = value[0:1]
    spots = row_spots(lanes())
    for m in range(4):
        for tile in range(2 if m < 3 else 1):
            rows = slice(8 * tile, 8 * tile + 8)
            for v in range(5):
                y, z_of = spots[v]
                got = take(acc_s[m, 1, rows, :], y)
                for z in range(2, 8):
                    got = jnp.where(z_of == z, take(acc_s[m, z, rows, :], y), got)
                grid_ref[m, rows, 128 * v : 128 * v + 128] = got
    grid_ref[3, 8:16, :] = jnp.zeros((8, 640), F32)
    out_copy.wait()


def end_kernel(
    za_ref, zb_ref, f_ref, vh_ref, inner_ref, v_out, a_out, a_s, v_s, acc_s, grid_s, sems
):
    at = lax.axis_index("gz")
    odd = at % 2 == 1
    outer = (at > 0) & (at < lax.axis_size("gz") - 1)
    spots = row_spots(lanes())

    def added(m, z, tile):
        at = (m * 9 + z) * XPAD + 8 * tile
        rows = slice(XPAD * m + 8 * tile, XPAD * m + 8 * tile + 8)
        near = za_ref[rows, :]
        far = jnp.where(outer, zb_ref[rows, :], 0.0)
        return f_ref[at : at + 8, :] + (
            jnp.where(odd, near, far) if z == 0 else jnp.where(odd, far, near)
        )

    def to_rows(m, tile):
        rows = slice(8 * tile, 8 * tile + 8)
        for v in range(5):
            y, z_of = spots[v]
            cols = slice(128 * v, 128 * v + 128)
            got = jnp.where(z_of == 0, take(acc_s[m, 0, rows, :], y), inner_ref[m, rows, cols])
            got = jnp.where(z_of == 8, take(acc_s[m, 1, rows, :], y), got)
            grid_s[m, rows, cols] = got

    for z in (0, 8):
        for tile in range(3):
            mass = added(3, z, tile)
            for m in range(3):
                value = added(m, z, tile) / mass
                if tile < 2:
                    acc_s[m, z // 8, 8 * tile : 8 * tile + 8, :] = value
                else:
                    acc_s[3, z // 8, m : m + 1, :] = value[0:1]
    to_rows(3, 0)
    for m in range(3):
        to_rows(m, 0)
        to_rows(m, 1)
        for x in range(16):
            a_s[m, :, pl.ds(ROW * x, ROW)] = grid_s[m, x : x + 1, :ROW]
        a_s[m, :, pl.ds(ROW * 16, ROW)] = grid_s[3, m : m + 1, :ROW]
    a_copy = pltpu.make_async_copy(a_s.at[pl.ds(0, 3)], a_out, sems.at[0])
    a_copy.start()
    v_s[...] = vh_ref[...] + HALF * a_s[0:3]
    v_copy = pltpu.make_async_copy(v_s, v_out, sems.at[1])
    v_copy.start()
    a_copy.wait()
    v_copy.wait()


def swap(value, at, second):
    axes = ("gx", "gy", "gz")
    sizes = [lax.axis_size(axis) for axis in axes]
    other = 0 if at == 2 else 2
    pairs = []
    for index in np.ndindex(*sizes):
        target = list(index)
        if not second:
            target[at] ^= 1
        elif 0 < index[at] < sizes[at] - 1:
            target[at] = ((index[at] - 1) ^ 1) + 1
        else:
            target[other] ^= 1
        pairs.append(tuple(int(np.ravel_multi_index(i, sizes)) for i in (index, target)))
    return lax.ppermute(value, axes, pairs)


def body(displ, veloc, accel, node_index, inv_map, jac_weight, lame_first, shear_mod, density):
    f32 = functools.partial(jax.ShapeDtypeStruct, dtype=F32)
    flat = (3, 1, NODES)
    points = (125, 1, 128)
    tables = [jnp.asarray(table) for table in operator_tables()]
    scratch = [
        pltpu.VMEM(flat, F32), pltpu.VMEM((1, 1, 128), jnp.int32),
        pltpu.VMEM((9, 128, 128), F32),
        pltpu.VMEM((128, 128), F32), pltpu.VMEM((128, 128), F32),
        pltpu.VMEM((128, 128), F32), pltpu.VMEM((128, 128), F32),
        pltpu.VMEM((384, 384), BF16), pltpu.VMEM((256, 384), BF16),
        pltpu.VMEM((4, 16, 640), F32), pltpu.VMEM((3, 7, 24, 128), F32),
        pltpu.VMEM((3, 200, 128), F32), pltpu.VMEM((384, 384), F32), pltpu.VMEM((4, 1, NODES), F32),
        pltpu.VMEM((384, 384), BF16), pltpu.VMEM((384, 384), BF16),
        pltpu.SemaphoreType.DMA((25,)),
    ]
    terms, slots, ya, v_old, a_old, displ_new = pl.pallas_call(
        force_kernel,
        out_shape=(
            f32((4, 200, 128)), jax.ShapeDtypeStruct((8, 128), jnp.int32), f32((XPAD, 128)),
            f32(flat), f32(flat), f32(flat),
        ),
        in_specs=[HBM] * 11,
        out_specs=(VMEM,) * 6,
        scratch_shapes=scratch,
        compiler_params=pltpu.CompilerParams(vmem_limit_bytes=16 << 20),
    )(
        *(
            pltpu.with_memory_space_constraint(value, pltpu.HBM)
            for value in (
                displ.reshape(flat), veloc.reshape(flat), accel.reshape(flat),
                node_index.reshape(points), inv_map.reshape(1125, 1, 128),
                jac_weight.reshape(points), lame_first.reshape(points), shear_mod.reshape(points),
                density.reshape(points), *tables,
            )
        )
    )
    small = pltpu.CompilerParams(vmem_limit_bytes=8 << 20)
    count = lax.axis_size("gy")
    hops = [(i, (i - 2) % count if i % 2 == 0 else (i + 2) % count) for i in range(count)]
    passed = lax.ppermute(ya, "gy", hops)
    field = pl.pallas_call(
        field_kernel,
        out_shape=f32((FROWS, 128)),
        in_specs=[VMEM] * 2,
        out_specs=VMEM,
        compiler_params=small,
        cost_estimate=pl.CostEstimate(flops=4000000, bytes_accessed=800000, transcendentals=0),
    )(terms, slots)
    passed, field = lax.optimization_barrier((passed, field))
    ya = swap(jnp.where(lanes((XPAD, 128)) < 64, ya, passed), 1, False)
    face = f32((40, 128))
    xa, xb = pl.pallas_call(
        x_kernel,
        out_shape=(face, face),
        in_specs=[VMEM] * 2,
        out_specs=(VMEM,) * 2,
        compiler_params=small,
    )(ya, field)
    field = pl.pallas_call(
        y_kernel,
        out_shape=f32((FROWS, 128)),
        in_specs=[VMEM] * 2,
        out_specs=VMEM,
        input_output_aliases={1: 0},
        compiler_params=small,
        cost_estimate=pl.CostEstimate(flops=1000000, bytes_accessed=800000, transcendentals=0),
    )(ya, field)
    xa = swap(xa, 0, False)
    xb = swap(xb, 0, True)
    face = f32((96, 128))
    field, za, zb = pl.pallas_call(
        z_kernel,
        out_shape=(f32((FROWS, 128)), face, face),
        in_specs=[VMEM] * 3,
        out_specs=(VMEM,) * 3,
        input_output_aliases={2: 0},
        compiler_params=pltpu.CompilerParams(vmem_limit_bytes=8 << 20),
    )(xa, xb, field)
    za = swap(za, 2, False)
    zb = swap(zb, 2, True)
    inner, v_half, displ_out = pl.pallas_call(
        inner_kernel,
        out_shape=(f32((4, 16, 640)), f32(flat), f32(flat)),
        in_specs=[VMEM] * 4,
        out_specs=(VMEM, VMEM, HBM),
        scratch_shapes=[pltpu.VMEM((4, 9, 16, 128), F32), pltpu.SemaphoreType.DMA],
        compiler_params=small,
        cost_estimate=pl.CostEstimate(flops=1000000, bytes_accessed=800000, transcendentals=0),
    )(field, displ_new, v_old, a_old)
    veloc_out, accel_out = pl.pallas_call(
        end_kernel,
        out_shape=(f32(flat), f32(flat)),
        in_specs=[VMEM] * 5,
        out_specs=(HBM, HBM),
        scratch_shapes=[
            pltpu.VMEM((4, 1, NODES), F32), pltpu.VMEM(flat, F32), pltpu.VMEM((4, 2, 16, 128), F32),
            pltpu.VMEM((4, 16, 640), F32), pltpu.SemaphoreType.DMA((2,)),
        ],
        compiler_params=pltpu.CompilerParams(vmem_limit_bytes=8 << 20),
    )(za, zb, field, v_half, inner)
    shape = (3, 1, 1, 1, NODES)
    return displ_out.reshape(shape), veloc_out.reshape(shape), accel_out.reshape(shape)


def solution(mesh):
    nodal = P(None, "gx", "gy", "gz", None)
    point = P("gx", "gy", "gz", None, None)
    placed = (nodal,) * 3 + (point, P("gx", "gy", "gz", None, None, None)) + (point,) * 4
    return jax.shard_map(
        body, mesh=mesh, in_specs=placed, out_specs=(nodal,) * 3, check_vma=False
    )
```
